128 devices in a mesh: fsdp: 2 (over core), ep: 64 (over z, y, x).
Axes of the slice: x: 4, y: 4, z: 4, core: 2. Of those that a mesh axis runs over, the one named last changes fastest.
Arguments:
- layer_in: bfloat16 [65536, 896], P(('fsdp', 'ep'))
- out_grad: bfloat16 [65536, 896], P(('fsdp', 'ep'))
- expert_ids: int32 [65536, 8], P(('fsdp', 'ep'))
- gate_vals: float32 [65536, 8], P(('fsdp', 'ep'))
- w_one: bfloat16 [64, 896, 640], P('ep', 'fsdp')
- w_two: bfloat16 [64, 640, 896], P('ep', None, 'fsdp')
- w_three: bfloat16 [64, 896, 640], P('ep', 'fsdp')
Outputs:
- output 1: bfloat16 [65536, 896], P(('fsdp', 'ep'))
- output 2: float32 [65536, 8], P(('fsdp', 'ep'))
- output 3: float32 [64, 896, 640], P('ep', 'fsdp')
- output 4: float32 [64, 640, 896], P('ep', None, 'fsdp')
- output 5: float32 [64, 896, 640], P('ep', 'fsdp')
All inputs are finite; a program needn't handle non-finite values.
Results may differ from the reference program's by a relative error of at most 0.0103469.
Values are sent between devices in bfloat16 or wider.
A program may use at most 1 GiB of HBM per device.

```python
import jax
import jax.numpy as jnp
from jax import lax

HIDDEN = 896
EXPERT_FF = 640
EXPERTS = 64
TOP_K = 8
TOKENS_DEV = 512
SHARDS = 128
CAPACITY = 80
TOKENS = SHARDS * TOKENS_DEV


def draw_routing(key):
    key_bias, key_hot, key_noise = jax.random.split(key, 3)
    noise_range = 65536
    spread = noise_range * TOP_K // (2 * EXPERTS)
    bias = jax.random.randint(key_bias, (EXPERTS,), 0, spread + 1)
    hot_expert = jax.random.randint(key_hot, (), 0, EXPERTS)
    expert_pos = jnp.arange(EXPERTS, dtype=jnp.int32)
    bias = bias + jnp.where(expert_pos == hot_expert, noise_range // 4, 0)
    noise = jax.random.randint(key_noise, (TOKENS, EXPERTS), 0, noise_range)
    scores = (noise + bias[None, :]) * EXPERTS + expert_pos[None, :]
    return lax.top_k(scores, TOP_K)[1].astype(jnp.int32)


def setup_inputs(seed: int = 0) -> dict:
    keys = jax.random.split(jax.random.key(seed), 7)
    layer_in = jax.random.normal(keys[0], (TOKENS, HIDDEN), jnp.float32).astype(jnp.bfloat16)
    out_grad = jax.random.normal(keys[1], (TOKENS, HIDDEN), jnp.float32).astype(jnp.bfloat16)
    expert_ids = draw_routing(keys[2])
    gate_vals = jax.random.uniform(keys[3], (TOKENS, TOP_K), jnp.float32, 0.25, 1.0)
    w_one = (jax.random.normal(keys[4], (EXPERTS, HIDDEN, EXPERT_FF), jnp.float32) * HIDDEN ** -0.5).astype(jnp.bfloat16)
    w_two = (jax.random.normal(keys[5], (EXPERTS, EXPERT_FF, HIDDEN), jnp.float32) * EXPERT_FF ** -0.5).astype(jnp.bfloat16)
    w_three = (jax.random.normal(keys[6], (EXPERTS, HIDDEN, EXPERT_FF), jnp.float32) * HIDDEN ** -0.5).astype(jnp.bfloat16)
    return {"layer_in": layer_in, "out_grad": out_grad, "expert_ids": expert_ids, "gate_vals": gate_vals, "w_one": w_one, "w_two": w_two, "w_three": w_three}


def reference(layer_in, out_grad, expert_ids, gate_vals, w_one, w_two, w_three):
    w_one_full = w_one.astype(jnp.float32)
    w_two_full = w_two.astype(jnp.float32)
    w_three_full = w_three.astype(jnp.float32)
    places = EXPERTS * CAPACITY
    expert_pos = jnp.arange(EXPERTS, dtype=jnp.int32)
    token_of = jnp.arange(TOKENS_DEV * TOP_K, dtype=jnp.int32) // TOP_K

    def shard_step(carry, shard):
        x_loc, dy_loc, ids_loc, gates_loc = shard
        flat_ids = ids_loc.reshape(-1)
        onehot = (flat_ids[:, None] == expert_pos[None, :]).astype(jnp.int32)
        before = jnp.cumsum(onehot, axis=0) - onehot
        position = jnp.sum(before * onehot, axis=1)
        slot_of = jnp.where(position < CAPACITY, flat_ids * CAPACITY + position, places)
        source = jnp.full((places,), TOKENS_DEV, jnp.int32).at[slot_of].set(token_of, mode="drop")
        slot_gate = jnp.zeros((places,), jnp.float32).at[slot_of].set(gates_loc.reshape(-1), mode="drop")
        x_buf = jnp.take(x_loc, source, axis=0, mode="fill", fill_value=0).reshape(EXPERTS, CAPACITY, HIDDEN).astype(jnp.float32)
        dy_buf = jnp.take(dy_loc, source, axis=0, mode="fill", fill_value=0).reshape(EXPERTS, CAPACITY, HIDDEN).astype(jnp.float32)
        h_one = jnp.einsum("ecd,edf->ecf", x_buf, w_one_full)
        h_three = jnp.einsum("ecd,edf->ecf", x_buf, w_three_full)
        sig_one = jax.nn.sigmoid(h_one)
        silu_one = h_one * sig_one
        act_bf = (silu_one * h_three).astype(jnp.bfloat16).astype(jnp.float32)
        y_buf = jnp.einsum("ecf,efd->ecd", act_bf, w_two_full)
        gate_buf = jnp.sum(dy_buf * y_buf, axis=-1)
        g_buf = (slot_gate.reshape(EXPERTS, CAPACITY, 1) * dy_buf).astype(jnp.bfloat16).astype(jnp.float32)
        d_act = jnp.einsum("ecd,efd->ecf", g_buf, w_two_full)
        dh_one = (d_act * h_three * sig_one * (1.0 + h_one * (1.0 - sig_one))).astype(jnp.bfloat16).astype(jnp.float32)
        dh_three = (d_act * silu_one).astype(jnp.bfloat16).astype(jnp.float32)
        dx_buf = (jnp.einsum("ecf,edf->ecd", dh_one, w_one_full) + jnp.einsum("ecf,edf->ecd", dh_three, w_three_full)).astype(jnp.bfloat16)
        dx_pick = jnp.take(dx_buf.reshape(places, HIDDEN), slot_of, axis=0, mode="fill", fill_value=0).reshape(TOKENS_DEV, TOP_K, HIDDEN)
        dx_tok = jnp.sum(dx_pick.astype(jnp.float32), axis=1).astype(jnp.bfloat16)
        gate_tok = jnp.take(gate_buf.reshape(places), slot_of, axis=0, mode="fill", fill_value=0).reshape(TOKENS_DEV, TOP_K)
        acc_one, acc_two, acc_three = carry
        acc_one = acc_one + jnp.einsum("ecd,ecf->edf", x_buf, dh_one)
        acc_two = acc_two + jnp.einsum("ecf,ecd->efd", act_bf, g_buf)
        acc_three = acc_three + jnp.einsum("ecd,ecf->edf", x_buf, dh_three)
        return (acc_one, acc_two, acc_three), (dx_tok, gate_tok)

    init = (jnp.zeros((EXPERTS, HIDDEN, EXPERT_FF), jnp.float32), jnp.zeros((EXPERTS, EXPERT_FF, HIDDEN), jnp.float32), jnp.zeros((EXPERTS, HIDDEN, EXPERT_FF), jnp.float32))
    shards = (layer_in.reshape(SHARDS, TOKENS_DEV, HIDDEN), out_grad.reshape(SHARDS, TOKENS_DEV, HIDDEN), expert_ids.reshape(SHARDS, TOKENS_DEV, TOP_K), gate_vals.reshape(SHARDS, TOKENS_DEV, TOP_K))
    (grad_one, grad_two, grad_three), (in_grad, gate_grad) = lax.scan(shard_step, init, shards)
    return in_grad.reshape(TOKENS, HIDDEN), gate_grad.reshape(TOKENS, TOP_K), grad_one, grad_two, grad_three
```

```python
import functools

import jax
import jax.numpy as jnp
from jax import lax
from jax.experimental import pallas as pl
from jax.experimental.pallas import tpu as pltpu
from jax.sharding import PartitionSpec as P

MESH = pl.DeviceIdType.MESH
ROWS = 16
BF16 = jnp.bfloat16
F32 = jnp.float32


def capacity_of(tok_dev, top_k, experts):
    return max(8, ((tok_dev * top_k * 5) // (4 * experts) + 7) // 8 * 8)


def column_groups(width):
    tiles = width // 128
    base = tiles // 3
    sizes = (base, base, tiles - 2 * base)
    starts = (0, base, 2 * base)
    return tuple((128 * s, 128 * n) for s, n in zip(starts, sizes))


def wait_bytes(ref, sem):
    pltpu.make_async_copy(ref, ref, sem).wait()


def dot(a, b, dims=((1,), (0,))):
    return lax.dot_general(a, b, (dims, ((), ())), preferred_element_type=F32)


def moe_kernel(ring, cap, x_hbm, u_hbm, ids_ref, gates_ref, w1_hbm, w3_hbm, w2_hbm,
               dx_out, dg_out, g1_out, g3_out, g2_out, mid_hbm, fin_hbm, b1_hbm, b2_hbm, b3_hbm,
               xa, pos0, pos1, pos2, line0, line1, line2, sg0, sg1, sg2, sg3, dg0, dg1, dg2, dg3,
               gbuf, xv, dxb, bv, acc, w1, w3, w2, dw1, dw3, dw2, dw1r, dw3r, dw2r,
               ld_s, ag_s, ag_r, p_s, p_r, w_s, w_r, sg_s, sg_r, dg_s, dg_r,
               s2_s, s2_r, s2_l, s3_s, s3_r, r1_s, r1_r, r1_l, r2_s, r2_r, r3_s, r3_r,
               cl_s, bl_s, dw_s, dw_r, out_s):
    tok, hidden = x_hbm.shape
    top_k = ids_ref.shape[0]
    half = w2_hbm.shape[1]
    chunks = cap // ROWS
    plane = ring * ring
    block = plane * ROWS
    cols = [pl.ds(s, n) for s, n in column_groups(hidden)]
    pos = (pos0, pos1, pos2)
    line = (line0, line1, line2)
    strides = (ring * ring, ring, 1)
    me = lax.axis_index("ep")
    core = lax.axis_index("fsdp")
    other = {"fsdp": 1 - core}
    coord = [lax.rem(me // s, ring) for s in strides]
    rest = pl.ds(1, ring - 1)

    def peer(axis, d):
        c = coord[axis]
        return {"ep": me + (lax.rem(c + d, ring) - c) * strides[axis]}

    def at(ref, lead, sel, col):
        return ref.at[(*lead, *(sel.get(a, slice(None)) for a in range(3)), slice(None), col)]

    def send(src, dst, s_sem, r_sem, device):
        pltpu.make_async_remote_copy(src_ref=src, dst_ref=dst, send_sem=s_sem, recv_sem=r_sem,
                                     device_id=device, device_id_type=MESH).start()

    def expert_column(order):
        row = lax.broadcasted_iota(jnp.int32, (ring ** 3, 1), 0)
        digits = (row // (ring * ring), lax.rem(row // ring, ring), lax.rem(row, ring))
        total = jnp.zeros_like(row)
        for digit, axis in zip(digits, order):
            total = total + lax.rem(digit + coord[axis], ring) * strides[axis]
        return total

    own = [
        pltpu.make_async_copy(x_hbm, xa.at[0, 0], ld_s.at[0]),
        pltpu.make_async_copy(u_hbm, xa.at[1, 0], ld_s.at[1]),
        pltpu.make_async_copy(w1_hbm, w1.at[core], ld_s.at[2]),
        pltpu.make_async_copy(w3_hbm, w3.at[core], ld_s.at[3]),
        pltpu.make_async_copy(w2_hbm, w2.at[core], ld_s.at[4]),
    ]
    for copy in own:
        copy.start()

    barrier = pltpu.get_barrier_semaphore()
    for axis in range(3):
        for d in range(1, ring):
            pl.semaphore_signal(barrier, inc=1, device_id=peer(axis, d), device_id_type=MESH)
    pl.semaphore_signal(barrier, inc=1, device_id=other, device_id_type=MESH)
    pl.semaphore_wait(barrier, 3 * (ring - 1) + 1)

    def gather_line(array, ref):
        for d in range(1, ring):
            for p in range(3):
                send(ref.at[:, cols[p]], xa.at[array, ring - d, :, cols[p]],
                     ag_s.at[array, p], ag_r.at[array, p], peer(p, d))

    gather_line(0, x_hbm)
    for i, (src, dst) in enumerate(((w1_hbm, w1), (w3_hbm, w3), (w2_hbm, w2))):
        send(src, dst.at[core], w_s.at[i], w_r.at[i], other)

    earlier = (lax.broadcasted_iota(jnp.int32, (tok, tok), 0) < lax.broadcasted_iota(jnp.int32, (tok, tok), 1))
    earlier = jnp.where(earlier, 1.0, 0.0).astype(BF16)
    for p, order in enumerate(((0, 1, 2), (1, 0, 2), (2, 0, 1))):
        expert = expert_column(order)
        chosen = jnp.zeros((ring ** 3, tok), F32)
        for j in range(top_k):
            chosen = chosen + jnp.where(ids_ref[j:j + 1, :] == expert, 1.0, 0.0)
        before = dot(chosen.astype(BF16), earlier)
        place = jnp.where((chosen > 0.5) & (before < cap), before, -1.0)
        pos[p][...] = place.reshape(ring, plane, tok)
        for d in range(1, ring):
            send(pos[p].at[d], line[p].at[ring - d], p_s.at[p], p_r.at[p], peer(p, d))
    gather_line(1, u_hbm)

    expert = expert_column((0, 1, 2))
    place = pos0[...].reshape(ring ** 3, tok)
    gate = jnp.zeros((ring ** 3, tok), F32)
    for j in range(top_k):
        gate = gate + jnp.where(ids_ref[j:j + 1, :] == expert, gates_ref[j:j + 1, :], 0.0)
    lane = lax.broadcasted_iota(jnp.int32, (ring ** 3, 128), 1)

    def gate_place(r, table):
        picked = jnp.sum(jnp.where(place == r.astype(F32), gate, 0.0), axis=1, keepdims=True)
        return jnp.where(lane == r, picked, table)

    table = lax.fori_loop(0, cap, gate_place, jnp.zeros((ring ** 3, 128), F32))
    sg0[...] = table.reshape(ring, ring, ring, 1, 128)

    def small_start(axis, src, dst, s_sem, r_sem):
        sel = lambda i: tuple(i if a == axis else slice(None) for a in range(3))
        for d in range(1, ring):
            send(src.at[sel(d)], dst.at[sel(ring - d)], s_sem.at[axis], r_sem.at[axis], peer(axis, d))
        dst[sel(pl.ds(0, 1))] = src[sel(pl.ds(0, 1))]

    def small_wait(axis, dst, r_sem):
        wait_bytes(dst.at[tuple(rest if a == axis else slice(None) for a in range(3))], r_sem.at[axis])

    small_start(0, sg0, sg1, sg_s, sg_r)
    for ref in (dw1, dw3, dw2, acc, dg0):
        ref[...] = jnp.zeros_like(ref)
    for copy in own:
        copy.wait()
    for p in range(3):
        wait_bytes(line[p].at[rest], p_r.at[p])

    def one_hot(places, first):
        n = places.shape[0]
        row = lax.broadcasted_iota(jnp.int32, (n, ROWS, tok), 1) + first
        hit = places[:, None, :] == row.astype(F32)
        return jnp.where(hit, 1.0, 0.0).astype(BF16).reshape(n * ROWS, tok)

    def dispatch(c):
        slot = lax.rem(c, 2)
        for array in range(2):
            for p in range(3):
                axis = (p + 1) % 3

                @pl.when(c == 0)
                def _():
                    wait_bytes(xa.at[array, rest, :, cols[p]], ag_r.at[array, p])

                @pl.when(c >= 2)
                def _():
                    wait_bytes(at(gbuf, (array, slot), {axis: rest}, cols[p]), s2_s.at[array, slot, p])

                width = column_groups(hidden)[p][1]
                for d in range(ring):
                    places = pos[p][0] if d == 0 else line[p][d]
                    rows = dot(one_hot(places, c * ROWS), xa[array, d, :, cols[p]]).astype(BF16)
                    idx = tuple(d if a == p else slice(None) for a in range(3))
                    gbuf[(array, slot, *idx, slice(None), cols[p])] = rows.reshape(ring, ring, ROWS, width)
                for d in range(1, ring):
                    send(at(gbuf, (array, slot), {axis: d}, cols[p]),
                         at(mid_hbm, (array, c), {axis: ring - d}, cols[p]),
                         s2_s.at[array, slot, p], s2_r.at[array, c, p], peer(axis, d))
                pltpu.make_async_copy(at(gbuf, (array, slot), {axis: 0}, cols[p]),
                                      at(mid_hbm, (array, c), {axis: 0}, cols[p]), s2_l.at[array, c, p]).start()

    def forward(c):
        for array in range(2):
            for p in range(3):
                axis, last = (p + 1) % 3, (p + 2) % 3
                wait_bytes(at(mid_hbm, (array, c), {axis: rest}, cols[p]), s2_r.at[array, c, p])
                wait_bytes(at(mid_hbm, (array, c), {axis: 0}, cols[p]), s2_l.at[array, c, p])
                for d in range(1, ring):
                    send(at(mid_hbm, (array, c), {last: d}, cols[p]),
                         at(fin_hbm, (array, c), {last: ring - d}, cols[p]),
                         s3_s.at[array, c, p], s3_r.at[array, c, p], peer(last, d))

    def compute(c):
        slot = lax.rem(c, 2)
        for array in range(2):
            for p in range(3):
                last = (p + 2) % 3
                wait_bytes(at(fin_hbm, (array, c), {last: rest}, cols[p]), s3_r.at[array, c, p])
                for src, part in ((fin_hbm, rest), (mid_hbm, 0)):
                    pltpu.make_async_copy(at(src, (array, c), {last: part}, cols[p]),
                                          at(xv, (array,), {last: part}, cols[p]), cl_s.at[array, p]).start()

        @pl.when(c >= 2)
        def _():
            for p in range(3):
                wait_bytes(at(dxb, (slot,), {(p + 2) % 3: rest}, cols[p]), r1_s.at[slot, p])

        for array in range(2):
            for p in range(3):
                wait_bytes(at(xv, (array,), {}, cols[p]), cl_s.at[array, p])

        def step(m, carry):
            x = xv[0, m].reshape(block, hidden)
            u = xv[1, m].reshape(block, hidden)
            w1_full = w1[...].reshape(hidden, -1)
            w3_full = w3[...].reshape(hidden, -1)
            hit = (lax.broadcasted_iota(jnp.int32, (plane, ROWS, 128), 2)
                   == lax.broadcasted_iota(jnp.int32, (plane, ROWS, 128), 1) + c * ROWS)
            s = jnp.sum(jnp.where(hit, sg3[m].reshape(plane, 1, 128), 0.0), axis=2, keepdims=True).reshape(block, 1)
            h1 = dot(x, w1_full)
            h3 = dot(x, w3_full)
            sig = jax.nn.sigmoid(h1)
            silu = h1 * sig
            act = (silu * h3).astype(BF16)
            u32 = u.astype(F32)
            g = (s * u32).astype(BF16)
            da = jnp.zeros_like(h1)
            dg = jnp.zeros((block, 1), F32)
            for i in range(2):
                span = slice(i * half, (i + 1) * half)
                g_half = g[:, span]
                y = dot(act, w2[i])
                dg = dg + jnp.sum(u32[:, span] * y, axis=1, keepdims=True)
                da = da + dot(g_half, w2[i], ((1,), (1,)))
                dw2[i] += dot(act, g_half, ((0,), (0,)))
            dh1 = (da * h3 * sig * (1.0 + h1 * (1.0 - sig))).astype(BF16)
            dh3 = (da * silu).astype(BF16)
            dx = dot(dh1, w1_full, ((1,), (1,))) + dot(dh3, w3_full, ((1,), (1,)))
            dxb[slot, m] = dx.astype(BF16).reshape(ring, ring, ROWS, hidden)
            dw1[...] += dot(x, dh1, ((0,), (0,))).reshape(dw1.shape)
            dw3[...] += dot(x, dh3, ((0,), (0,))).reshape(dw3.shape)
            spread = jnp.sum(jnp.where(hit, dg.reshape(plane, ROWS, 1), 0.0), axis=1, keepdims=True)
            dg0[m] += spread.reshape(ring, ring, 1, 128)
            return carry

        lax.fori_loop(0, ring, step, 0)
        for p in range(3):
            last = (p + 2) % 3
            for d in range(1, ring):
                send(at(dxb, (slot,), {last: d}, cols[p]), at(b1_hbm, (c,), {last: ring - d}, cols[p]),
                     r1_s.at[slot, p], r1_r.at[c, p], peer(last, d))
            pltpu.make_async_copy(at(dxb, (slot,), {last: 0}, cols[p]), at(b1_hbm, (c,), {last: 0}, cols[p]),
                                  r1_l.at[c, p]).start()

    def back_two(c):
        for p in range(3):
            axis, last = (p + 1) % 3, (p + 2) % 3
            wait_bytes(at(b1_hbm, (c,), {last: rest}, cols[p]), r1_r.at[c, p])
            wait_bytes(at(b1_hbm, (c,), {last: 0}, cols[p]), r1_l.at[c, p])
            for d in range(1, ring):
                send(at(b1_hbm, (c,), {axis: d}, cols[p]), at(b2_hbm, (c,), {axis: ring - d}, cols[p]),
                     r2_s.at[c, p], r2_r.at[c, p], peer(axis, d))

    def back_three(c):
        for p in range(3):
            axis = (p + 1) % 3
            wait_bytes(at(b2_hbm, (c,), {axis: rest}, cols[p]), r2_r.at[c, p])
            for d in range(1, ring):
                for src, part in ((b2_hbm, rest), (b1_hbm, 0)):
                    send(at(src, (c,), {p: d, axis: part}, cols[p]),
                         at(b3_hbm, (c,), {p: ring - d, axis: part}, cols[p]),
                         r3_s.at[c, p], r3_r.at[c, p], peer(p, d))

    def combine(c):
        for p in range(3):
            axis = (p + 1) % 3
            wait_bytes(at(b3_hbm, (c,), {p: rest}, cols[p]), r3_r.at[c, p])
            for src, sel in ((b3_hbm, {p: rest}), (b2_hbm, {p: 0, axis: rest}), (b1_hbm, {p: 0, axis: 0})):
                pltpu.make_async_copy(at(src, (c,), sel, cols[p]), at(bv, (), sel, cols[p]), bl_s.at[p]).start()
        for p in range(3):
            wait_bytes(at(bv, (), {}, cols[p]), bl_s.at[p])

        def step(m, carry):
            acc[...] += dot(one_hot(pos0[m], c * ROWS), bv[m].reshape(block, hidden), ((0,), (0,)))
            return carry

        lax.fori_loop(0, ring, step, 0)

    grads = ((dw1, dw1r, g1_out), (dw3, dw3r, g3_out), (dw2, dw2r, g2_out))

    def gate_grads():
        small_wait(0, dg3, dg_r)
        expert = expert_column((0, 1, 2))
        place = pos0[...].reshape(ring ** 3, tok)
        values = dg3[...].reshape(ring ** 3, 128)

        def pick(r, total):
            value = jnp.sum(jnp.where(lane == r, values, 0.0), axis=1, keepdims=True)
            return total + jnp.where(place == r.astype(F32), value, 0.0)

        dense = lax.fori_loop(0, cap, pick, jnp.zeros((ring ** 3, tok), F32))
        for j in range(top_k):
            dg_out[j:j + 1, :] = jnp.sum(jnp.where(ids_ref[j:j + 1, :] == expert, dense, 0.0), axis=0, keepdims=True)

    def tick(k, carry):
        @pl.when(k < chunks)
        def _():
            dispatch(k)

        @pl.when(k == 0)
        def _():
            small_wait(0, sg1, sg_r)
            small_start(1, sg1, sg2, sg_s, sg_r)

        @pl.when(k == 1)
        def _():
            small_wait(1, sg2, sg_r)
            small_start(2, sg2, sg3, sg_s, sg_r)

        @pl.when((k >= 1) & (k <= chunks))
        def _():
            forward(k - 1)

        @pl.when((k >= 4) & (k < chunks + 4))
        def _():
            back_three(k - 4)

        @pl.when((k >= 3) & (k < chunks + 3))
        def _():
            back_two(k - 3)

        @pl.when(k == 2)
        def _():
            small_wait(2, sg3, sg_r)
            for i, ref in enumerate((w1, w3, w2)):
                wait_bytes(ref.at[1 - core], w_r.at[i])

        @pl.when((k >= 2) & (k < chunks + 2))
        def _():
            compute(k - 2)

        @pl.when(k == chunks + 1)
        def _():
            small_start(2, dg0, dg1, dg_s, dg_r)
            for i, (mine, theirs, _) in enumerate(grads):
                send(mine.at[1 - core], theirs, dw_s.at[i], dw_r.at[i], other)

        @pl.when(k == chunks + 2)
        def _():
            small_wait(2, dg1, dg_r)
            small_start(1, dg1, dg2, dg_s, dg_r)
            for i, (mine, theirs, out) in enumerate(grads):
                wait_bytes(theirs, dw_r.at[i])
                theirs[...] += mine[core]
                pltpu.make_async_copy(theirs, out, out_s.at[i]).start()

        @pl.when(k == chunks + 3)
        def _():
            small_wait(1, dg2, dg_r)
            small_start(0, dg2, dg3, dg_s, dg_r)

        @pl.when(k == chunks + 4)
        def _():
            gate_grads()

        @pl.when(k >= 5)
        def _():
            combine(k - 5)

        return carry

    lax.fori_loop(0, chunks + 5, tick, 0)
    dx_out[...] = acc[...].astype(BF16)

    for array in range(2):
        for p in range(3):
            wait_bytes(xa.at[array, rest, :, cols[p]], ag_s.at[array, p])
    for p in range(3):
        wait_bytes(line[p].at[rest], p_s.at[p])
        wait_bytes(sg1.at[rest], sg_s.at[p])
        wait_bytes(dg1.at[rest], dg_s.at[p])
    for i, ref in enumerate((w1, w3, w2)):
        wait_bytes(ref.at[1 - core], w_s.at[i])
    for i, (mine, theirs, out) in enumerate(grads):
        wait_bytes(theirs, dw_s.at[i])
        wait_bytes(out, out_s.at[i])
    for slot in range(2):
        for p in range(3):
            axis, last = (p + 1) % 3, (p + 2) % 3
            for array in range(2):
                wait_bytes(at(gbuf, (array, slot), {axis: rest}, cols[p]), s2_s.at[array, slot, p])
            wait_bytes(at(dxb, (slot,), {last: rest}, cols[p]), r1_s.at[slot, p])

    def drain(c, carry):
        for p in range(3):
            axis, last = (p + 1) % 3, (p + 2) % 3
            for array in range(2):
                wait_bytes(at(fin_hbm, (array, c), {last: rest}, cols[p]), s3_s.at[array, c, p])
            wait_bytes(at(b2_hbm, (c,), {axis: rest}, cols[p]), r2_s.at[c, p])
            wait_bytes(at(b3_hbm, (c,), {p: rest}, cols[p]), r3_s.at[c, p])
        return carry

    lax.fori_loop(0, chunks, drain, 0)


def build(mesh, capacity=None):
    ep_size = mesh.shape["ep"]
    ring = round(ep_size ** (1 / 3))
    tok_spec = P(("fsdp", "ep"), None)
    up_spec = P("ep", "fsdp", None)
    down_spec = P("ep", None, "fsdp")

    def per_device(layer_in, out_grad, expert_ids, gate_vals, w_one, w_two, w_three):
        tok, hidden = layer_in.shape
        top_k = expert_ids.shape[1]
        _, half, width = w_one.shape
        cap = capacity or capacity_of(tok, top_k, ep_size)
        chunks = cap // ROWS
        cube = (ring, ring, ring, ROWS, hidden)
        table = (ring, ring * ring, tok)
        small = (ring, ring, ring, 1, 128)
        vmem, dma = pltpu.VMEM, pltpu.SemaphoreType.DMA
        hbm = pl.BlockSpec(memory_space=pl.ANY)
        local = pl.BlockSpec(memory_space=pltpu.VMEM)
        sds = jax.ShapeDtypeStruct
        outs = pl.pallas_call(
            functools.partial(moe_kernel, ring, cap),
            out_shape=[
                sds((tok, hidden), BF16), sds((top_k, tok), F32),
                sds((half, width), F32), sds((half, width), F32), sds((width, half), F32),
                sds((2, chunks, *cube), BF16), sds((2, chunks, *cube), BF16),
                sds((chunks, *cube), BF16), sds((chunks, *cube), BF16), sds((chunks, *cube), BF16),
            ],
            in_specs=[hbm, hbm, local, local, hbm, hbm, hbm],
            out_specs=[local, local] + [hbm] * 8,
            scratch_shapes=[
                vmem((2, ring, tok, hidden), BF16),
                *[vmem(table, F32)] * 6,
                *[vmem(small, F32)] * 8,
                vmem((2, 2, *cube), BF16), vmem((2, *cube), BF16), vmem((2, *cube), BF16), vmem(cube, BF16),
                vmem((tok, hidden), F32),
                vmem((2, half, width), BF16), vmem((2, half, width), BF16), vmem((2, width, half), BF16),
                vmem((2, half, width), F32), vmem((2, half, width), F32), vmem((2, width, half), F32),
                vmem((half, width), F32), vmem((half, width), F32), vmem((width, half), F32),
                dma((5,)), dma((2, 3)), dma((2, 3)), dma((3,)), dma((3,)), dma((3,)), dma((3,)),
                dma((3,)), dma((3,)), dma((3,)), dma((3,)),
                dma((2, 2, 3)), dma((2, chunks, 3)), dma((2, chunks, 3)),
                dma((2, chunks, 3)), dma((2, chunks, 3)),
                dma((2, 3)), dma((chunks, 3)), dma((chunks, 3)),
                dma((chunks, 3)), dma((chunks, 3)), dma((chunks, 3)), dma((chunks, 3)),
                dma((2, 3)), dma((3,)), dma((3,)), dma((3,)), dma((3,)),
            ],
            compiler_params=pltpu.CompilerParams(
                collective_id=0, has_side_effects=True, vmem_limit_bytes=63 << 20
            ),
            name="moe_backward",
        )(layer_in, out_grad, expert_ids.T, gate_vals.T, w_one[0], w_three[0], w_two[0])
        dx, dg, g1, g3, g2 = outs[:5]
        return dx, dg.T, g1[None], g2[None], g3[None]

    return jax.shard_map(per_device, mesh=mesh,
                         in_specs=(tok_spec, tok_spec, tok_spec, tok_spec, up_spec, down_spec, up_spec),
                         out_specs=(tok_spec, tok_spec, up_spec, down_spec, up_spec), check_vma=False)


def solution(mesh):
    return build(mesh)
```

```python
import functools

import jax
import jax.numpy as jnp
from jax import lax
from jax.experimental import pallas as pl
from jax.experimental.pallas import tpu as pltpu
from jax.sharding import PartitionSpec as P

MESH = pl.DeviceIdType.MESH
ROWS = 16
BF16 = jnp.bfloat16
F32 = jnp.float32


def capacity_of(tok_dev, top_k, experts):
    return max(8, ((tok_dev * top_k * 5) // (4 * experts) + 7) // 8 * 8)


def column_groups(width, wide):
    tiles = width // 128
    base = tiles // 3
    sizes = [base + (tiles - 3 * base if p == wide else 0) for p in range(3)]
    starts = [sum(sizes[:p]) for p in range(3)]
    return [(128 * s, 128 * n) for s, n in zip(starts, sizes)]


def wait_bytes(ref, sem):
    pltpu.make_async_copy(ref, ref, sem).wait()


def dot(a, b, dims=((1,), (0,))):
    return lax.dot_general(a, b, (dims, ((), ())), preferred_element_type=F32)


def at(ref, lead, sel, col):
    return ref.at[(*lead, *(sel.get(a, slice(None)) for a in range(3)), slice(None), col)]


def one_hot(places, first):
    n, tok = places.shape
    row = lax.broadcasted_iota(jnp.int32, (n, ROWS, tok), 1) + first
    hit = places[:, None, :] == row.astype(F32)
    return jnp.where(hit, 1.0, 0.0).astype(BF16).reshape(n * ROWS, tok)


def returned_parts(ring, p):
    axis, rest = (p + 1) % 3, pl.ds(1, ring - 1)
    return ({p: 0, axis: 0}, {p: 0, axis: rest}, {p: rest})


def moe_kernel(ring, cap, x_hbm, u_hbm, ids_ref, gates_ref, w1_hbm, w3_hbm, w2_hbm,
               dg_out, acc_out, pos_out, g1_out, g3_out, g2_out, mid_hbm, fin_hbm, b1_hbm, b2_hbm, b3_hbm,
               xa, pos0, pos1, pos2, line0, line1, line2, sg0, sg1, sg2, sg3, dg0, dg1, dg2, dg3,
               gbuf, xv, dxb, bv, acc, w13, w2, dw13, dw2, dw1r, dw3r, dw2r,
               ld_s, ag_s, ag_r, far_s, far_r, p_s, p_r, w_s, w_r, sg_s, sg_r, dg_s, dg_r,
               s2_s, s2_r, s2_l, s3_s, s3_r, r1_s, r1_r, r1_l, r2_s, r2_r, r3_s, r3_r,
               cl_s, bl_s, dw_s, dw_r, out_s, end_s):
    tok, hidden = x_hbm.shape
    top_k = ids_ref.shape[0]
    chunks = cap // ROWS
    plane = ring * ring
    block = plane * ROWS
    send_cols = [[pl.ds(s, n) for s, n in column_groups(hidden, wide)] for wide in (2, 0)]
    cols = [pl.ds(s, n) for s, n in column_groups(hidden, 1)]
    pos = (pos0, pos1, pos2)
    line = (line0, line1, line2)
    strides = (ring * ring, ring, 1)
    me = lax.axis_index("ep")
    core = lax.axis_index("fsdp")
    other = {"fsdp": 1 - core}
    coord = [lax.rem(me // s, ring) for s in strides]
    rest = pl.ds(1, ring - 1)
    width = w1_hbm.shape[1]
    one, three = pl.ds(0, width), pl.ds(width, width)
    weights = (lambda i: w13.at[i, :, one], lambda i: w13.at[i, :, three], lambda i: w2.at[i])

    def peer(axis, d):
        c = coord[axis]
        return {"ep": me + (lax.rem(c + d, ring) - c) * strides[axis]}

    def send(src, dst, s_sem, r_sem, device):
        pltpu.make_async_remote_copy(src_ref=src, dst_ref=dst, send_sem=s_sem, recv_sem=r_sem,
                                     device_id=device, device_id_type=MESH).start()

    def expert_column(order):
        row = lax.broadcasted_iota(jnp.int32, (ring ** 3, 1), 0)
        digits = (row // (ring * ring), lax.rem(row // ring, ring), lax.rem(row, ring))
        total = jnp.zeros_like(row)
        for digit, axis in zip(digits, order):
            total = total + lax.rem(digit + coord[axis], ring) * strides[axis]
        return total

    own = [
        pltpu.make_async_copy(x_hbm, xa.at[0, 0], ld_s.at[0]),
        pltpu.make_async_copy(u_hbm, xa.at[1, 0], ld_s.at[1]),
        pltpu.make_async_copy(w1_hbm, weights[0](core), ld_s.at[2]),
        pltpu.make_async_copy(w3_hbm, weights[1](core), ld_s.at[3]),
        pltpu.make_async_copy(w2_hbm, weights[2](core), ld_s.at[4]),
    ]
    for copy in own:
        copy.start()

    barrier = pltpu.get_barrier_semaphore()
    for axis in range(3):
        for d in range(1, ring):
            pl.semaphore_signal(barrier, inc=1, device_id=peer(axis, d), device_id_type=MESH)
    pl.semaphore_signal(barrier, inc=1, device_id=other, device_id_type=MESH)

    earlier = (lax.broadcasted_iota(jnp.int32, (tok, tok), 0) < lax.broadcasted_iota(jnp.int32, (tok, tok), 1))
    earlier = jnp.where(earlier, 1.0, 0.0).astype(BF16)
    for p, order in enumerate(((0, 1, 2), (1, 0, 2), (2, 0, 1))):
        expert = expert_column(order)
        chosen = jnp.zeros((ring ** 3, tok), F32)
        for j in range(top_k):
            chosen = chosen + jnp.where(ids_ref[j:j + 1, :] == expert, 1.0, 0.0)
        before = dot(chosen.astype(BF16), earlier)
        place = jnp.where((chosen > 0.5) & (before < cap), before, -1.0)
        pos[p][...] = place.reshape(ring, plane, tok)

    pltpu.make_async_copy(pos0, pos_out, end_s.at[0]).start()
    pl.semaphore_wait(barrier, 3 * (ring - 1) + 1)

    for p in range(3):
        for d in range(1, ring):
            send(pos[p].at[d], line[p].at[ring - d], p_s.at[p], p_r.at[p], peer(p, d))

    sides = sorted({1, ring - 1})

    def gather_line(array, ref):
        for d in sides:
            for p in range(3):
                send(ref.at[:, send_cols[array][p]], xa.at[array, ring - d, :, send_cols[array][p]],
                     ag_s.at[array, p, d // 2], ag_r.at[array, p, (ring - d) // 2], peer(p, d))

    gather_line(0, x_hbm)
    gather_line(1, u_hbm)
    for i, src in enumerate((w1_hbm, w3_hbm, w2_hbm)):
        send(src, weights[i](core), w_s.at[i], w_r.at[i], other)

    expert = expert_column((0, 1, 2))
    place = pos0[...].reshape(ring ** 3, tok)
    gate = jnp.zeros((ring ** 3, tok), F32)
    for j in range(top_k):
        gate = gate + jnp.where(ids_ref[j:j + 1, :] == expert, gates_ref[j:j + 1, :], 0.0)
    lane = lax.broadcasted_iota(jnp.int32, (ring ** 3, 128), 1)

    def gate_place(i, table):
        for j in range(8):
            r = 8 * i + j
            picked = jnp.sum(jnp.where(place == r.astype(F32), gate, 0.0), axis=1, keepdims=True)
            table = jnp.where(lane == r, picked, table)
        return table

    table = lax.fori_loop(0, cap // 8, gate_place, jnp.zeros((ring ** 3, 128), F32))
    sg0[...] = table.reshape(ring, ring, ring, 1, 128)

    def small_start(axis, src, dst, s_sem, r_sem):
        sel = lambda i: tuple(i if a == axis else slice(None) for a in range(3))
        for d in range(1, ring):
            send(src.at[sel(d)], dst.at[sel(ring - d)], s_sem.at[axis], r_sem.at[axis], peer(axis, d))
        dst[sel(pl.ds(0, 1))] = src[sel(pl.ds(0, 1))]

    def small_wait(axis, dst, r_sem):
        wait_bytes(dst.at[tuple(rest if a == axis else slice(None) for a in range(3))], r_sem.at[axis])

    small_start(0, sg0, sg1, sg_s, sg_r)
    for ref in (dw13, dw2, acc, dg0):
        ref[...] = jnp.zeros_like(ref)
    for array in range(2):
        for d in sides:
            for p in range(3):
                col = send_cols[array][p]
                wait_bytes(xa.at[array, d, :, col], ag_r.at[array, p, d // 2])
                if ring == 4:
                    part = pl.ds((d // 2) * (tok // 2), tok // 2)
                    send(xa.at[array, d, part, col], xa.at[array, 2, part, col],
                         far_s.at[array, p], far_r.at[array, p], peer(p, ring - d))
    for copy in own:
        copy.wait()
    for p in range(3):
        wait_bytes(line[p].at[rest], p_r.at[p])

    def dispatch(c):
        slot = lax.rem(c, 2)
        for array in range(2):
            for p in range(3):
                axis = (p + 1) % 3

                if ring == 4:
                    @pl.when(c == 0)
                    def _():
                        wait_bytes(xa.at[array, 2, :, send_cols[array][p]], far_r.at[array, p])

                @pl.when(c >= 2)
                def _():
                    wait_bytes(at(gbuf, (array, slot), {axis: rest}, send_cols[array][p]), s2_s.at[array, slot, p])

                width = send_cols[array][p].size
                for d in range(ring):
                    places = pos[p][0] if d == 0 else line[p][d]
                    rows = dot(one_hot(places, c * ROWS), xa[array, d, :, send_cols[array][p]]).astype(BF16)
                    idx = tuple(d if a == p else slice(None) for a in range(3))
                    gbuf[(array, slot, *idx, slice(None), send_cols[array][p])] = rows.reshape(ring, ring, ROWS, width)
                for d in range(1, ring):
                    send(at(gbuf, (array, slot), {axis: d}, send_cols[array][p]),
                         at(mid_hbm, (array, c), {axis: ring - d}, send_cols[array][p]),
                         s2_s.at[array, slot, p], s2_r.at[array, c, p], peer(axis, d))
                pltpu.make_async_copy(at(gbuf, (array, slot), {axis: 0}, send_cols[array][p]),
                                      at(mid_hbm, (array, c), {axis: 0}, send_cols[array][p]), s2_l.at[array, c, p]).start()

    def forward(c):
        for array in range(2):
            for p in range(3):
                axis, last = (p + 1) % 3, (p + 2) % 3
                wait_bytes(at(mid_hbm, (array, c), {axis: rest}, send_cols[array][p]), s2_r.at[array, c, p])
                wait_bytes(at(mid_hbm, (array, c), {axis: 0}, send_cols[array][p]), s2_l.at[array, c, p])
                for d in range(1, ring):
                    send(at(mid_hbm, (array, c), {last: d}, send_cols[array][p]),
                         at(fin_hbm, (array, c), {last: ring - d}, send_cols[array][p]),
                         s3_s.at[array, c, p], s3_r.at[array, c, p], peer(last, d))

    def compute(c):
        slot = lax.rem(c, 2)
        for array in range(2):
            for p in range(3):
                last = (p + 2) % 3
                wait_bytes(at(fin_hbm, (array, c), {last: rest}, send_cols[array][p]), s3_r.at[array, c, p])
                for src, part in ((fin_hbm, rest), (mid_hbm, 0)):
                    pltpu.make_async_copy(at(src, (array, c), {last: part}, send_cols[array][p]),
                                          at(xv, (array,), {last: part}, send_cols[array][p]), cl_s.at[array, p]).start()

        @pl.when(c >= 2)
        def _():
            for p in range(3):
                wait_bytes(at(dxb, (slot,), {(p + 2) % 3: rest}, cols[p]), r1_s.at[slot, p])

        for array in range(2):
            for p in range(3):
                wait_bytes(at(xv, (array,), {}, send_cols[array][p]), cl_s.at[array, p])

        def step(i, carry):
            slabs = pl.ds(2 * i, 2)
            x = xv[0, slabs].reshape(2 * block, hidden)
            u = xv[1, slabs].reshape(2 * block, hidden)
            w13_full = w13[...].reshape(hidden, 2 * width)
            hit = (lax.broadcasted_iota(jnp.int32, (2 * plane, ROWS, 128), 2)
                   == lax.broadcasted_iota(jnp.int32, (2 * plane, ROWS, 128), 1) + c * ROWS)
            s = sg3[slabs].reshape(2 * plane, 1, 128)
            s = jnp.sum(jnp.where(hit, s, 0.0), axis=2, keepdims=True).reshape(2 * block, 1)
            h13 = dot(x, w13_full)
            h1, h3 = h13[:, :width], h13[:, width:]
            sig = jax.nn.sigmoid(h1)
            silu = h1 * sig
            act = (silu * h3).astype(BF16)
            u32 = u.astype(F32)
            g = (s * u32).astype(BF16)
            w2_full = w2[...].reshape(hidden, width)
            y = dot(act, w2_full, ((1,), (1,)))
            dg = jnp.sum(u32 * y, axis=1, keepdims=True)
            da = dot(g, w2_full)
            dw2[...] += dot(g, act, ((0,), (0,))).reshape(dw2.shape)
            dh1 = (da * h3 * sig * (1.0 + h1 * (1.0 - sig))).astype(BF16)
            dh3 = (da * silu).astype(BF16)
            dh13 = jnp.concatenate([dh1, dh3], axis=1)
            dx = dot(dh13, w13_full, ((1,), (1,)))
            dxb[slot, slabs] = dx.astype(BF16).reshape(2, ring, ring, ROWS, hidden)
            dw13[...] += dot(x, dh13, ((0,), (0,))).reshape(dw13.shape)
            spread = jnp.sum(jnp.where(hit, dg.reshape(2 * plane, ROWS, 1), 0.0), axis=1, keepdims=True)
            dg0[slabs] += spread.reshape(2, ring, ring, 1, 128)
            for j in range(2):
                return_slab(2 * i + j)
            return carry

        def return_slab(m):
            for p in range(3):
                last = (p + 2) % 3

                def start(here, there, device):
                    src, dst = at(dxb, (slot,), here, cols[p]), at(b1_hbm, (c,), there, cols[p])
                    if device is None:
                        pltpu.make_async_copy(src, dst, r1_l.at[c, p]).start()
                    else:
                        send(src, dst, r1_s.at[slot, p], r1_r.at[c, p], device)

                if last == 0:
                    @pl.when(m > 0)
                    def _():
                        start({0: m}, {0: ring - m}, peer(0, m))

                    @pl.when(m == 0)
                    def _():
                        start({0: 0}, {0: 0}, None)
                else:
                    for d in range(1, ring):
                        start({0: m, last: d}, {0: m, last: ring - d}, peer(last, d))
                    start({0: m, last: 0}, {0: m, last: 0}, None)

        lax.fori_loop(0, ring // 2, step, 0)

    def back_two(c):
        for p in range(3):
            axis, last = (p + 1) % 3, (p + 2) % 3
            wait_bytes(at(b1_hbm, (c,), {last: rest}, cols[p]), r1_r.at[c, p])
            wait_bytes(at(b1_hbm, (c,), {last: 0}, cols[p]), r1_l.at[c, p])
            for d in range(1, ring):
                send(at(b1_hbm, (c,), {axis: d}, cols[p]), at(b2_hbm, (c,), {axis: ring - d}, cols[p]),
                     r2_s.at[c, p], r2_r.at[c, p], peer(axis, d))

    def back_three(c):
        for p in range(3):
            axis = (p + 1) % 3
            wait_bytes(at(b2_hbm, (c,), {axis: rest}, cols[p]), r2_r.at[c, p])
            for d in range(1, ring):
                for src, part in ((b2_hbm, rest), (b1_hbm, 0)):
                    send(at(src, (c,), {p: d, axis: part}, cols[p]),
                         at(b3_hbm, (c,), {p: ring - d, axis: part}, cols[p]),
                         r3_s.at[c, p], r3_r.at[c, p], peer(p, d))

    def combine(c):
        for p in range(3):
            wait_bytes(at(b3_hbm, (c,), {p: rest}, cols[p]), r3_r.at[c, p])
            for src, sel in zip((b1_hbm, b2_hbm, b3_hbm), returned_parts(ring, p)):
                pltpu.make_async_copy(at(src, (c,), sel, cols[p]), at(bv, (), sel, cols[p]), bl_s.at[p]).start()
        for p in range(3):
            wait_bytes(at(bv, (), {}, cols[p]), bl_s.at[p])

        def step(m, carry):
            acc[...] += dot(one_hot(pos0[m], c * ROWS), bv[m].reshape(block, hidden), ((0,), (0,)))
            return carry

        lax.fori_loop(0, ring, step, 0)

    grads = (
        (lambda i: dw13.at[i, :, one], dw1r, g1_out),
        (lambda i: dw13.at[i, :, three], dw3r, g3_out),
        (lambda i: dw2.at[i], dw2r, g2_out),
    )

    def gate_grads():
        small_wait(0, dg3, dg_r)
        expert = expert_column((0, 1, 2))
        place = pos0[...].reshape(ring ** 3, tok)
        values = dg3[...].reshape(ring ** 3, 128)

        def pick(i, total):
            for j in range(8):
                r = 8 * i + j
                value = jnp.sum(jnp.where(lane == r, values, 0.0), axis=1, keepdims=True)
                total = total + jnp.where(place == r.astype(F32), value, 0.0)
            return total

        dense = lax.fori_loop(0, cap // 8, pick, jnp.zeros((ring ** 3, tok), F32))
        for j in range(top_k):
            dg_out[j:j + 1, :] = jnp.sum(jnp.where(ids_ref[j:j + 1, :] == expert, dense, 0.0), axis=0, keepdims=True)

    def tick(k, carry):
        @pl.when(k < chunks)
        def _():
            dispatch(k)

        @pl.when(k == 0)
        def _():
            small_wait(0, sg1, sg_r)
            small_start(1, sg1, sg2, sg_s, sg_r)

        @pl.when(k == 1)
        def _():
            small_wait(1, sg2, sg_r)
            small_start(2, sg2, sg3, sg_s, sg_r)

        @pl.when((k >= 1) & (k <= chunks))
        def _():
            forward(k - 1)

        @pl.when(k == 2)
        def _():
            small_wait(2, sg3, sg_r)
            for i in range(3):
                wait_bytes(weights[i](1 - core), w_r.at[i])

        @pl.when(k >= 2)
        def _():
            compute(k - 2)

        @pl.when(k >= 3)
        def _():
            back_two(k - 3)

        @pl.when(k >= 4)
        def _():
            back_three(k - 4)

        @pl.when((k >= 5) & (k <= chunks))
        def _():
            combine(k - 5)

        return carry

    lax.fori_loop(0, chunks + 2, tick, 0)
    last_one = chunks - 1
    small_start(2, dg0, dg1, dg_s, dg_r)
    for i, (mine, theirs, _) in enumerate(grads):
        send(mine(1 - core), theirs, dw_s.at[i], dw_r.at[i], other)
    back_two(last_one)
    combine(last_one - 3)
    back_three(last_one - 1)
    small_wait(2, dg1, dg_r)
    small_start(1, dg1, dg2, dg_s, dg_r)
    combine(last_one - 2)
    back_three(last_one)
    small_wait(1, dg2, dg_r)
    small_start(0, dg2, dg3, dg_s, dg_r)
    for i, (mine, theirs, out) in enumerate(grads):
        wait_bytes(theirs, dw_r.at[i])
        theirs[...] += mine(core)[...]
        pltpu.make_async_copy(theirs, out, out_s.at[i]).start()
    combine(last_one - 1)
    pltpu.make_async_copy(acc, acc_out, end_s.at[1]).start()
    gate_grads()

    for array in range(2):
        for p in range(3):
            for d in sides:
                wait_bytes(xa.at[array, d, :, send_cols[array][p]], ag_s.at[array, p, d // 2])
            if ring == 4:
                wait_bytes(xa.at[array, 2, :, send_cols[array][p]], far_s.at[array, p])
    for p in range(3):
        wait_bytes(line[p].at[rest], p_s.at[p])
        wait_bytes(sg1.at[rest], sg_s.at[p])
        wait_bytes(dg1.at[rest], dg_s.at[p])
    for i in range(3):
        wait_bytes(weights[i](1 - core), w_s.at[i])
    for i, (mine, theirs, out) in enumerate(grads):
        wait_bytes(theirs, dw_s.at[i])
        wait_bytes(out, out_s.at[i])
    for slot in range(2):
        for p in range(3):
            axis, last = (p + 1) % 3, (p + 2) % 3
            for array in range(2):
                wait_bytes(at(gbuf, (array, slot), {axis: rest}, send_cols[array][p]), s2_s.at[array, slot, p])
            wait_bytes(at(dxb, (slot,), {last: rest}, cols[p]), r1_s.at[slot, p])

    def drain(c, carry):
        for p in range(3):
            axis, last = (p + 1) % 3, (p + 2) % 3
            for array in range(2):
                wait_bytes(at(fin_hbm, (array, c), {last: rest}, send_cols[array][p]), s3_s.at[array, c, p])
            wait_bytes(at(b2_hbm, (c,), {axis: rest}, cols[p]), r2_s.at[c, p])
            wait_bytes(at(b3_hbm, (c,), {p: rest}, cols[p]), r3_s.at[c, p])
        return carry

    lax.fori_loop(0, chunks, drain, 0)
    wait_bytes(pos_out, end_s.at[0])
    wait_bytes(acc_out, end_s.at[1])
    for p in range(3):
        wait_bytes(at(b3_hbm, (last_one,), {p: rest}, cols[p]), r3_r.at[last_one, p])


def finish_kernel(ring, cap, acc_hbm, pos_hbm, g1_hbm, g3_hbm, g2_hbm, b1_hbm, b2_hbm, b3_hbm,
                  dx_hbm, g1_out, g3_out, g2_out, acc, pos, grad, bv, dx, in_s, out_s):
    hidden = acc.shape[1]
    chunk = cap // ROWS - 1
    cols = [pl.ds(s, n) for s, n in column_groups(hidden, 1)]
    pltpu.make_async_copy(pos_hbm, pos, in_s.at[0]).start()
    for p in range(3):
        for src, sel in zip((b1_hbm, b2_hbm, b3_hbm), returned_parts(ring, p)):
            pltpu.make_async_copy(at(src, (chunk,), sel, cols[p]), at(bv, (), sel, cols[p]), in_s.at[1]).start()
    pltpu.make_async_copy(acc_hbm, acc, in_s.at[2]).start()
    for i, src in enumerate((g1_hbm, g3_hbm, g2_hbm)):
        pltpu.make_async_copy(src, grad.at[i], in_s.at[3 + i]).start()
    wait_bytes(pos, in_s.at[0])
    wait_bytes(bv, in_s.at[1])
    wait_bytes(acc, in_s.at[2])
    for m in range(ring):
        block = ring * ring * ROWS
        acc[...] += dot(one_hot(pos[m], chunk * ROWS), bv[m].reshape(block, hidden), ((0,), (0,)))
        if m < 3:
            wait_bytes(grad.at[m], in_s.at[3 + m])
            pltpu.make_async_copy(grad.at[m], (g1_out, g3_out, g2_out)[m], out_s.at[m]).start()
    for m in range(ring, 3):
        wait_bytes(grad.at[m], in_s.at[3 + m])
        pltpu.make_async_copy(grad.at[m], (g1_out, g3_out, g2_out)[m], out_s.at[m]).start()
    dx[...] = acc[...].astype(BF16)
    copy = pltpu.make_async_copy(dx, dx_hbm, out_s.at[3])
    copy.start()
    for m, out in enumerate((g1_out, g3_out, g2_out)):
        wait_bytes(out, out_s.at[m])
    copy.wait()


def build(mesh, capacity=None):
    ep_size = mesh.shape["ep"]
    ring = round(ep_size ** (1 / 3))
    tok_spec = P(("fsdp", "ep"), None)
    up_spec = P("ep", "fsdp", None)
    down_spec = P("ep", None, "fsdp")

    def per_device(layer_in, out_grad, expert_ids, gate_vals, w_one, w_two, w_three):
        tok, hidden = layer_in.shape
        top_k = expert_ids.shape[1]
        _, half, width = w_one.shape
        cap = capacity or capacity_of(tok, top_k, ep_size)
        chunks = cap // ROWS
        cube = (ring, ring, ring, ROWS, hidden)
        table = (ring, ring * ring, tok)
        small = (ring, ring, ring, 1, 128)
        vmem, dma = pltpu.VMEM, pltpu.SemaphoreType.DMA
        hbm = pl.BlockSpec(memory_space=pl.ANY)
        local = pl.BlockSpec(memory_space=pltpu.VMEM)
        sds = jax.ShapeDtypeStruct
        outs = pl.pallas_call(
            functools.partial(moe_kernel, ring, cap),
            out_shape=[
                sds((top_k, tok), F32), sds((tok, hidden), F32), sds(table, F32),
                *[sds((half, width), F32)] * 3,
                sds((2, chunks, *cube), BF16), sds((2, chunks, *cube), BF16),
                sds((chunks, *cube), BF16), sds((chunks, *cube), BF16), sds((chunks, *cube), BF16),
            ],
            in_specs=[hbm, hbm, local, local, hbm, hbm, hbm],
            out_specs=[local] + [hbm] * 10,
            scratch_shapes=[
                vmem((2, ring, tok, hidden), BF16),
                *[vmem(table, F32)] * 6,
                *[vmem(small, F32)] * 8,
                vmem((2, 2, *cube), BF16), vmem((2, *cube), BF16), vmem((2, *cube), BF16), vmem(cube, BF16),
                vmem((tok, hidden), F32),
                vmem((2, half, 2 * width), BF16), vmem((2, half, width), BF16),
                vmem((2, half, 2 * width), F32), vmem((2, half, width), F32),
                *[vmem((half, width), F32)] * 3,
                dma((5,)), dma((2, 3, 2)), dma((2, 3, 2)), dma((2, 3)), dma((2, 3)), dma((3,)), dma((3,)), dma((3,)), dma((3,)),
                dma((3,)), dma((3,)), dma((3,)), dma((3,)),
                dma((2, 2, 3)), dma((2, chunks, 3)), dma((2, chunks, 3)),
                dma((2, chunks, 3)), dma((2, chunks, 3)),
                dma((2, 3)), dma((chunks, 3)), dma((chunks, 3)),
                dma((chunks, 3)), dma((chunks, 3)), dma((chunks, 3)), dma((chunks, 3)),
                dma((2, 3)), dma((3,)), dma((3,)), dma((3,)), dma((3,)), dma((2,)),
            ],
            compiler_params=pltpu.CompilerParams(
                collective_id=0, has_side_effects=True, vmem_limit_bytes=63 << 20
            ),
            name="moe_backward",
        )(layer_in, out_grad, expert_ids.T, gate_vals.T, w_one[0], w_three[0], w_two[0].T)
        dg, acc, places, g1, g3, g2 = outs[:6]
        dx, g1, g3, g2 = pl.pallas_call(
            functools.partial(finish_kernel, ring, cap),
            out_shape=[sds((tok, hidden), BF16), *[sds((half, width), F32)] * 3],
            in_specs=[hbm] * 8,
            out_specs=[hbm] * 4,
            scratch_shapes=[
                vmem((tok, hidden), F32), vmem(table, F32), vmem((3, half, width), F32), vmem(cube, BF16),
                vmem((tok, hidden), BF16), dma((6,)), dma((4,)),
            ],
            compiler_params=pltpu.CompilerParams(vmem_limit_bytes=63 << 20),
            name="moe_finish",
        )(acc, places, g1, g3, g2, *outs[8:])
        return dx, dg.T, g1[None], g2.T[None], g3[None]

    return jax.shard_map(per_device, mesh=mesh,
                         in_specs=(tok_spec, tok_spec, tok_spec, tok_spec, up_spec, down_spec, up_spec),
                         out_specs=(tok_spec, tok_spec, up_spec, down_spec, up_spec), check_vma=False)


def solution(mesh):
    return build(mesh)
```

```python
import functools

import jax
import jax.numpy as jnp
from jax import lax
from jax.experimental import pallas as pl
from jax.experimental.pallas import tpu as pltpu
from jax.sharding import PartitionSpec as P

MESH = pl.DeviceIdType.MESH
ROWS = 16
BF16 = jnp.bfloat16
F32 = jnp.float32


def capacity_of(tok_dev, top_k, experts):
    return max(8, ((tok_dev * top_k * 5) // (4 * experts) + 7) // 8 * 8)


def column_groups(width, wide):
    tiles = width // 128
    base = tiles // 3
    sizes = [base + (tiles - 3 * base if p == wide else 0) for p in range(3)]
    starts = [sum(sizes[:p]) for p in range(3)]
    return [(128 * s, 128 * n) for s, n in zip(starts, sizes)]


def split_groups(width):
    base, spare = width // 384 * 128, width % 384
    even = [(0, base), (base, base), (2 * base, spare + base)]
    odd = [(0, base), (base, base + spare), (2 * base + spare, base)]
    return even, odd, (2 * base, spare)


def wait_bytes(ref, sem):
    pltpu.make_async_copy(ref, ref, sem).wait()


def dot(a, b, dims=((1,), (0,))):
    return lax.dot_general(a, b, (dims, ((), ())), preferred_element_type=F32)


def at(ref, lead, sel, col):
    return ref.at[(*lead, *(sel.get(a, slice(None)) for a in range(3)), slice(None), col)]


def one_hot(places, first):
    n, tok = places.shape
    row = lax.broadcasted_iota(jnp.int32, (n, ROWS, tok), 1) + first
    hit = places[:, None, :] == row.astype(F32)
    return jnp.where(hit, 1.0, 0.0).astype(BF16).reshape(n * ROWS, tok)


def returned_parts(ring, p):
    axis, rest = (p + 1) % 3, pl.ds(1, ring - 1)
    return ({p: 0, axis: 0}, {p: 0, axis: rest}, {p: rest})


def moe_kernel(ring, cap, x_hbm, u_hbm, ids_ref, gates_ref, w1_hbm, w3_hbm, w2_hbm,
               dg_out, acc_out, pos_out, g1_out, g3_out, g2_out, mid_hbm, fin_hbm, b1_hbm, b2_hbm, b3_hbm,
               xa, xe, pos0, pos1, pos2, line0, line1, line2, sg0, sg1, sg2, sg3, dg0, dg1, dg2, dg3,
               gbuf, xv, dxb, bv, acc, w13, w2, dw13, dw2, dw1r, dw3r, dw2r,
               ld_s, ag_s, ag_r, far_s, far_r, p_s, p_r, w_s, w_r, sg_s, sg_r, dg_s, dg_r,
               s2_s, s2_r, s2_l, s3_s, s3_r, r1_s, r1_r, r1_l, r2_s, r2_r, r3_s, r3_r,
               cl_s, bl_s, dw_s, dw_r, out_s, end_s):
    tok, hidden = x_hbm.shape
    top_k = ids_ref.shape[0]
    chunks = cap // ROWS
    plane = ring * ring
    block = plane * ROWS
    even, odd, spare = split_groups(hidden)
    spans = lambda groups: [pl.ds(s, n) for s, n in groups]
    even, odd, u_cols, cols = spans(even), spans(odd), spans(column_groups(hidden, 0)), spans(column_groups(hidden, 1))
    spare = pl.ds(*spare)
    pieces = [(0, 0, even[0]), (0, 1, even[1]), (0, 2, even[2])] + ([(0, 1, spare)] if spare.size else [])
    pieces += [(1, p, u_cols[p]) for p in range(3)]

    def held(i, d, part=slice(None), col=None):
        array, axis, whole = pieces[i]
        return xe.at[d, part] if i == 3 and spare.size else xa.at[array, d, part, col or whole]

    def by_chunk(array, c, body):
        if array == 1:
            body(u_cols)
        elif isinstance(c, int):
            body(odd if c % 2 else even)
        else:
            for parity, groups in enumerate((even, odd)):
                pl.when(lax.rem(c, 2) == parity)(functools.partial(body, groups))
    pos = (pos0, pos1, pos2)
    line = (line0, line1, line2)
    strides = (ring * ring, ring, 1)
    me = lax.axis_index("ep")
    core = lax.axis_index("fsdp")
    other = {"fsdp": 1 - core}
    coord = [lax.rem(me // s, ring) for s in strides]
    rest = pl.ds(1, ring - 1)
    width = w1_hbm.shape[1]
    one, three = pl.ds(0, width), pl.ds(width, width)
    weights = (lambda i: w13.at[i, :, one], lambda i: w13.at[i, :, three], lambda i: w2.at[i])

    def peer(axis, d):
        c = coord[axis]
        return {"ep": me + (lax.rem(c + d, ring) - c) * strides[axis]}

    def send(src, dst, s_sem, r_sem, device):
        pltpu.make_async_remote_copy(src_ref=src, dst_ref=dst, send_sem=s_sem, recv_sem=r_sem,
                                     device_id=device, device_id_type=MESH).start()

    def expert_column(order):
        row = lax.broadcasted_iota(jnp.int32, (ring ** 3, 1), 0)
        digits = (row // (ring * ring), lax.rem(row // ring, ring), lax.rem(row, ring))
        total = jnp.zeros_like(row)
        for digit, axis in zip(digits, order):
            total = total + lax.rem(digit + coord[axis], ring) * strides[axis]
        return total

    own = [
        pltpu.make_async_copy(x_hbm, xa.at[0, 0], ld_s.at[0]),
        pltpu.make_async_copy(u_hbm, xa.at[1, 0], ld_s.at[1]),
        *([pltpu.make_async_copy(x_hbm.at[:, spare], xe.at[0], ld_s.at[5])] if spare.size else []),
        pltpu.make_async_copy(w1_hbm, weights[0](core), ld_s.at[2]),
        pltpu.make_async_copy(w3_hbm, weights[1](core), ld_s.at[3]),
        pltpu.make_async_copy(w2_hbm, weights[2](core), ld_s.at[4]),
    ]
    for copy in own:
        copy.start()

    barrier = pltpu.get_barrier_semaphore()
    for axis in range(3):
        for d in range(1, ring):
            pl.semaphore_signal(barrier, inc=1, device_id=peer(axis, d), device_id_type=MESH)
    pl.semaphore_signal(barrier, inc=1, device_id=other, device_id_type=MESH)

    earlier = (lax.broadcasted_iota(jnp.int32, (tok, tok), 0) < lax.broadcasted_iota(jnp.int32, (tok, tok), 1))
    earlier = jnp.where(earlier, 1.0, 0.0).astype(BF16)
    for p, order in enumerate(((0, 1, 2), (1, 0, 2), (2, 0, 1))):
        expert = expert_column(order)
        chosen = jnp.zeros((ring ** 3, tok), F32)
        for j in range(top_k):
            chosen = chosen + jnp.where(ids_ref[j:j + 1, :] == expert, 1.0, 0.0)
        before = dot(chosen.astype(BF16), earlier)
        place = jnp.where((chosen > 0.5) & (before < cap), before, -1.0)
        pos[p][...] = place.reshape(ring, plane, tok)

    pltpu.make_async_copy(pos0, pos_out, end_s.at[0]).start()
    pl.semaphore_wait(barrier, 3 * (ring - 1) + 1)

    for p in range(3):
        for d in range(1, ring):
            send(pos[p].at[d], line[p].at[ring - d], p_s.at[p], p_r.at[p], peer(p, d))

    sides = sorted({1, ring - 1})

    for i, (array, axis, col) in enumerate(pieces):
        for d in sides:
            send((x_hbm, u_hbm)[array].at[:, col], held(i, ring - d), ag_s.at[i, d // 2], ag_r.at[i, (ring - d) // 2],
                 peer(axis, d))
    for i, src in enumerate((w1_hbm, w3_hbm, w2_hbm)):
        send(src, weights[i](core), w_s.at[i], w_r.at[i], other)

    expert = expert_column((0, 1, 2))
    place = pos0[...].reshape(ring ** 3, tok)
    gate = jnp.zeros((ring ** 3, tok), F32)
    for j in range(top_k):
        gate = gate + jnp.where(ids_ref[j:j + 1, :] == expert, gates_ref[j:j + 1, :], 0.0)
    lane = lax.broadcasted_iota(jnp.int32, (ring ** 3, 128), 1)

    def gate_place(i, table):
        for j in range(8):
            r = 8 * i + j
            picked = jnp.sum(jnp.where(place == r.astype(F32), gate, 0.0), axis=1, keepdims=True)
            table = jnp.where(lane == r, picked, table)
        return table

    table = lax.fori_loop(0, cap // 8, gate_place, jnp.zeros((ring ** 3, 128), F32))
    sg0[...] = table.reshape(ring, ring, ring, 1, 128)

    def small_start(axis, src, dst, s_sem, r_sem):
        sel = lambda i: tuple(i if a == axis else slice(None) for a in range(3))
        for d in range(1, ring):
            send(src.at[sel(d)], dst.at[sel(ring - d)], s_sem.at[axis], r_sem.at[axis], peer(axis, d))
        dst[sel(pl.ds(0, 1))] = src[sel(pl.ds(0, 1))]

    def small_wait(axis, dst, r_sem):
        wait_bytes(dst.at[tuple(rest if a == axis else slice(None) for a in range(3))], r_sem.at[axis])

    small_start(0, sg0, sg1, sg_s, sg_r)
    for ref in (dw13, dw2, acc, dg0):
        ref[...] = jnp.zeros_like(ref)
    for i, (array, axis, col) in enumerate(pieces):
        for d in sides:
            wait_bytes(held(i, d), ag_r.at[i, d // 2])
            if ring == 4:
                part = pl.ds((d // 2) * (tok // 2), tok // 2)
                send(held(i, d, part), held(i, 2, part), far_s.at[i], far_r.at[i], peer(axis, ring - d))
    for copy in own:
        copy.wait()
    for p in range(3):
        wait_bytes(line[p].at[rest], p_r.at[p])

    def dispatch(c):
        for array in range(2):
            by_chunk(array, c, functools.partial(dispatch_stream, c, array))

    def dispatch_stream(c, array, groups):
        slot = lax.rem(c, 2)
        for p in range(3):
            axis, col = (p + 1) % 3, groups[p]
            mine = [i for i, piece in enumerate(pieces) if piece[:2] == (array, p)]
            for i in mine:
                if ring == 4:
                    @pl.when(c == 0)
                    def _():
                        wait_bytes(held(i, 2), far_r.at[i])

            @pl.when(c >= 2)
            def _():
                wait_bytes(at(gbuf, (array, slot), {axis: rest}, col), s2_s.at[array, slot, p])

            for d in range(ring):
                hot = one_hot(pos[p][0] if d == 0 else line[p][d], c * ROWS)
                for i in mine:
                    first = max(pieces[i][2].start, col.start)
                    end = min(pieces[i][2].start + pieces[i][2].size, col.start + col.size)
                    if first >= end:
                        continue
                    own_col = pl.ds(first, end - first)
                    rows = dot(hot, held(i, d, col=own_col)[...]).astype(BF16)
                    idx = tuple(d if a == p else slice(None) for a in range(3))
                    gbuf[(array, slot, *idx, slice(None), own_col)] = rows.reshape(ring, ring, ROWS, own_col.size)
            for d in range(1, ring):
                send(at(gbuf, (array, slot), {axis: d}, col), at(mid_hbm, (array, c), {axis: ring - d}, col),
                     s2_s.at[array, slot, p], s2_r.at[array, c, p], peer(axis, d))
            pltpu.make_async_copy(at(gbuf, (array, slot), {axis: 0}, col),
                                  at(mid_hbm, (array, c), {axis: 0}, col), s2_l.at[array, c, p]).start()

    def forward(c):
        for array in range(2):
            by_chunk(array, c, functools.partial(forward_stream, c, array))

    def forward_stream(c, array, groups):
        for p, col in enumerate(groups):
            axis, last = (p + 1) % 3, (p + 2) % 3
            wait_bytes(at(mid_hbm, (array, c), {axis: rest}, col), s2_r.at[array, c, p])
            wait_bytes(at(mid_hbm, (array, c), {axis: 0}, col), s2_l.at[array, c, p])
            for d in range(1, ring):
                send(at(mid_hbm, (array, c), {last: d}, col), at(fin_hbm, (array, c), {last: ring - d}, col),
                     s3_s.at[array, c, p], s3_r.at[array, c, p], peer(last, d))

    def load_stream(c, array, groups):
        for p, col in enumerate(groups):
            last = (p + 2) % 3
            wait_bytes(at(fin_hbm, (array, c), {last: rest}, col), s3_r.at[array, c, p])
            for src, part in ((fin_hbm, rest), (mid_hbm, 0)):
                pltpu.make_async_copy(at(src, (array, c), {last: part}, col),
                                      at(xv, (array,), {last: part}, col), cl_s.at[array]).start()

    def compute(c):
        slot = lax.rem(c, 2)
        for array in range(2):
            by_chunk(array, c, functools.partial(load_stream, c, array))

        @pl.when(c >= 2)
        def _():
            for p in range(3):
                wait_bytes(at(dxb, (slot,), {(p + 2) % 3: rest}, cols[p]), r1_s.at[slot, p])

        for array in range(2):
            wait_bytes(xv.at[array], cl_s.at[array])

        def step(i, carry):
            slabs = pl.ds(2 * i, 2)
            x = xv[0, slabs].reshape(2 * block, hidden)
            u = xv[1, slabs].reshape(2 * block, hidden)
            w13_full = w13[...].reshape(hidden, 2 * width)
            hit = (lax.broadcasted_iota(jnp.int32, (2 * plane, ROWS, 128), 2)
                   == lax.broadcasted_iota(jnp.int32, (2 * plane, ROWS, 128), 1) + c * ROWS)
            s = sg3[slabs].reshape(2 * plane, 1, 128)
            s = jnp.sum(jnp.where(hit, s, 0.0), axis=2, keepdims=True).reshape(2 * block, 1)
            h13 = dot(x, w13_full)
            h1, h3 = h13[:, :width], h13[:, width:]
            sig = jax.nn.sigmoid(h1)
            silu = h1 * sig
            act = (silu * h3).astype(BF16)
            u32 = u.astype(F32)
            g = (s * u32).astype(BF16)
            w2_full = w2[...].reshape(hidden, width)
            y = dot(act, w2_full, ((1,), (1,)))
            dg = jnp.sum(u32 * y, axis=1, keepdims=True)
            da = dot(g, w2_full)
            dw2[...] += dot(g, act, ((0,), (0,))).reshape(dw2.shape)
            dh1 = (da * h3 * sig * (1.0 + h1 * (1.0 - sig))).astype(BF16)
            dh3 = (da * silu).astype(BF16)
            dh13 = jnp.concatenate([dh1, dh3], axis=1)
            dx = dot(dh13, w13_full, ((1,), (1,)))
            dxb[slot, slabs] = dx.astype(BF16).reshape(2, ring, ring, ROWS, hidden)
            dw13[...] += dot(x, dh13, ((0,), (0,))).reshape(dw13.shape)
            spread = jnp.sum(jnp.where(hit, dg.reshape(2 * plane, ROWS, 1), 0.0), axis=1, keepdims=True)
            dg0[slabs] += spread.reshape(2, ring, ring, 1, 128)
            for j in range(2):
                return_slab(2 * i + j)
            return carry

        def return_slab(m):
            for p in range(3):
                last = (p + 2) % 3

                def start(here, there, device):
                    src, dst = at(dxb, (slot,), here, cols[p]), at(b1_hbm, (c,), there, cols[p])
                    if device is None:
                        pltpu.make_async_copy(src, dst, r1_l.at[c, p]).start()
                    else:
                        send(src, dst, r1_s.at[slot, p], r1_r.at[c, p], device)

                if last == 0:
                    @pl.when(m > 0)
                    def _():
                        start({0: m}, {0: ring - m}, peer(0, m))

                    @pl.when(m == 0)
                    def _():
                        start({0: 0}, {0: 0}, None)
                else:
                    for d in range(1, ring):
                        start({0: m, last: d}, {0: m, last: ring - d}, peer(last, d))
                    start({0: m, last: 0}, {0: m, last: 0}, None)

        lax.fori_loop(0, ring // 2, step, 0)

    def back_two(c):
        for p in range(3):
            axis, last = (p + 1) % 3, (p + 2) % 3
            wait_bytes(at(b1_hbm, (c,), {last: rest}, cols[p]), r1_r.at[c, p])
            wait_bytes(at(b1_hbm, (c,), {last: 0}, cols[p]), r1_l.at[c, p])
            for d in range(1, ring):
                send(at(b1_hbm, (c,), {axis: d}, cols[p]), at(b2_hbm, (c,), {axis: ring - d}, cols[p]),
                     r2_s.at[c, p], r2_r.at[c, p], peer(axis, d))

    def back_three(c):
        for p in range(3):
            axis = (p + 1) % 3
            wait_bytes(at(b2_hbm, (c,), {axis: rest}, cols[p]), r2_r.at[c, p])
            for d in range(1, ring):
                for src, part in ((b2_hbm, rest), (b1_hbm, 0)):
                    send(at(src, (c,), {p: d, axis: part}, cols[p]),
                         at(b3_hbm, (c,), {p: ring - d, axis: part}, cols[p]),
                         r3_s.at[c, p], r3_r.at[c, p], peer(p, d))

    def combine(c):
        for p in range(3):
            wait_bytes(at(b3_hbm, (c,), {p: rest}, cols[p]), r3_r.at[c, p])
            for src, sel in zip((b1_hbm, b2_hbm, b3_hbm), returned_parts(ring, p)):
                pltpu.make_async_copy(at(src, (c,), sel, cols[p]), at(bv, (), sel, cols[p]), bl_s.at[p]).start()
        for p in range(3):
            wait_bytes(at(bv, (), {}, cols[p]), bl_s.at[p])

        def step(m, carry):
            acc[...] += dot(one_hot(pos0[m], c * ROWS), bv[m].reshape(block, hidden), ((0,), (0,)))
            return carry

        lax.fori_loop(0, ring, step, 0)

    grads = (
        (lambda i: dw13.at[i, :, one], dw1r, g1_out),
        (lambda i: dw13.at[i, :, three], dw3r, g3_out),
        (lambda i: dw2.at[i], dw2r, g2_out),
    )

    def gate_grads():
        small_wait(0, dg3, dg_r)
        expert = expert_column((0, 1, 2))
        place = pos0[...].reshape(ring ** 3, tok)
        values = dg3[...].reshape(ring ** 3, 128)

        def pick(i, total):
            for j in range(8):
                r = 8 * i + j
                value = jnp.sum(jnp.where(lane == r, values, 0.0), axis=1, keepdims=True)
                total = total + jnp.where(place == r.astype(F32), value, 0.0)
            return total

        dense = lax.fori_loop(0, cap // 8, pick, jnp.zeros((ring ** 3, tok), F32))
        for j in range(top_k):
            dg_out[j:j + 1, :] = jnp.sum(jnp.where(ids_ref[j:j + 1, :] == expert, dense, 0.0), axis=0, keepdims=True)

    def tick(k, carry):
        @pl.when(k < chunks)
        def _():
            dispatch(k)

        @pl.when(k == 0)
        def _():
            small_wait(0, sg1, sg_r)
            small_start(1, sg1, sg2, sg_s, sg_r)

        @pl.when(k == 1)
        def _():
            small_wait(1, sg2, sg_r)
            small_start(2, sg2, sg3, sg_s, sg_r)

        @pl.when((k >= 1) & (k <= chunks))
        def _():
            forward(k - 1)

        @pl.when(k == 2)
        def _():
            small_wait(2, sg3, sg_r)
            for i in range(3):
                wait_bytes(weights[i](1 - core), w_r.at[i])

        @pl.when(k >= 2)
        def _():
            compute(k - 2)

        @pl.when(k >= 3)
        def _():
            back_two(k - 3)

        @pl.when(k >= 4)
        def _():
            back_three(k - 4)

        @pl.when((k >= 5) & (k <= chunks))
        def _():
            combine(k - 5)

        return carry

    lax.fori_loop(0, chunks + 2, tick, 0)
    last_one = chunks - 1
    small_start(2, dg0, dg1, dg_s, dg_r)
    for i, (mine, theirs, _) in enumerate(grads):
        send(mine(1 - core), theirs, dw_s.at[i], dw_r.at[i], other)
    back_two(last_one)
    combine(last_one - 3)
    back_three(last_one - 1)
    small_wait(2, dg1, dg_r)
    small_start(1, dg1, dg2, dg_s, dg_r)
    combine(last_one - 2)
    back_three(last_one)
    small_wait(1, dg2, dg_r)
    small_start(0, dg2, dg3, dg_s, dg_r)
    for i, (mine, theirs, out) in enumerate(grads):
        wait_bytes(theirs, dw_r.at[i])
        theirs[...] += mine(core)[...]
        pltpu.make_async_copy(theirs, out, out_s.at[i]).start()
    combine(last_one - 1)
    pltpu.make_async_copy(acc, acc_out, end_s.at[1]).start()
    gate_grads()

    for i in range(len(pieces)):
        for d in sides:
            wait_bytes(held(i, d), ag_s.at[i, d // 2])
        if ring == 4:
            wait_bytes(held(i, 2), far_s.at[i])
    for p in range(3):
        wait_bytes(line[p].at[rest], p_s.at[p])
        wait_bytes(sg1.at[rest], sg_s.at[p])
        wait_bytes(dg1.at[rest], dg_s.at[p])
    for i in range(3):
        wait_bytes(weights[i](1 - core), w_s.at[i])
    for i, (mine, theirs, out) in enumerate(grads):
        wait_bytes(theirs, dw_s.at[i])
        wait_bytes(out, out_s.at[i])
    for slot in range(2):
        for p in range(3):
            axis, last = (p + 1) % 3, (p + 2) % 3
            for array in range(2):
                by_chunk(array, slot, lambda groups: wait_bytes(
                    at(gbuf, (array, slot), {axis: rest}, groups[p]), s2_s.at[array, slot, p]))
            wait_bytes(at(dxb, (slot,), {last: rest}, cols[p]), r1_s.at[slot, p])

    def drain(c, carry):
        for p in range(3):
            axis, last = (p + 1) % 3, (p + 2) % 3
            for array in range(2):
                by_chunk(array, c, lambda groups: wait_bytes(
                    at(fin_hbm, (array, c), {last: rest}, groups[p]), s3_s.at[array, c, p]))
            wait_bytes(at(b2_hbm, (c,), {axis: rest}, cols[p]), r2_s.at[c, p])
            wait_bytes(at(b3_hbm, (c,), {p: rest}, cols[p]), r3_s.at[c, p])
        return carry

    lax.fori_loop(0, chunks, drain, 0)
    wait_bytes(pos_out, end_s.at[0])
    wait_bytes(acc_out, end_s.at[1])
    for p in range(3):
        wait_bytes(at(b3_hbm, (last_one,), {p: rest}, cols[p]), r3_r.at[last_one, p])


def finish_kernel(ring, cap, dg_hbm, acc_hbm, pos_hbm, g1_hbm, g3_hbm, g2_hbm, b1_hbm, b2_hbm, b3_hbm,
                  dx_hbm, dg_out, g1_out, g3_out, g2_out, acc, pos, grad, bv, dx, dg, in_s, out_s):
    hidden = acc.shape[1]
    chunk = cap // ROWS - 1
    cols = [pl.ds(s, n) for s, n in column_groups(hidden, 1)]
    pltpu.make_async_copy(pos_hbm, pos, in_s.at[0]).start()
    for p in range(3):
        for src, sel in zip((b1_hbm, b2_hbm, b3_hbm), returned_parts(ring, p)):
            pltpu.make_async_copy(at(src, (chunk,), sel, cols[p]), at(bv, (), sel, cols[p]), in_s.at[1]).start()
    pltpu.make_async_copy(acc_hbm, acc, in_s.at[2]).start()
    for i, src in enumerate((g1_hbm, g3_hbm, g2_hbm)):
        pltpu.make_async_copy(src, grad.at[i], in_s.at[3 + i]).start()
    pltpu.make_async_copy(dg_hbm, dg, in_s.at[6]).start()
    wait_bytes(pos, in_s.at[0])
    wait_bytes(bv, in_s.at[1])
    wait_bytes(acc, in_s.at[2])
    for m in range(ring):
        block = ring * ring * ROWS
        acc[...] += dot(one_hot(pos[m], chunk * ROWS), bv[m].reshape(block, hidden), ((0,), (0,)))
        if m < 3:
            wait_bytes(grad.at[m], in_s.at[3 + m])
            pltpu.make_async_copy(grad.at[m], (g1_out, g3_out, g2_out)[m], out_s.at[m]).start()
    for m in range(ring, 3):
        wait_bytes(grad.at[m], in_s.at[3 + m])
        pltpu.make_async_copy(grad.at[m], (g1_out, g3_out, g2_out)[m], out_s.at[m]).start()
    wait_bytes(dg, in_s.at[6])
    pltpu.make_async_copy(dg, dg_out, out_s.at[4]).start()
    dx[...] = acc[...].astype(BF16)
    copy = pltpu.make_async_copy(dx, dx_hbm, out_s.at[3])
    copy.start()
    for m, out in enumerate((g1_out, g3_out, g2_out)):
        wait_bytes(out, out_s.at[m])
    wait_bytes(dg_out, out_s.at[4])
    copy.wait()


def build(mesh, capacity=None):
    ep_size = mesh.shape["ep"]
    ring = round(ep_size ** (1 / 3))
    tok_spec = P(("fsdp", "ep"), None)
    up_spec = P("ep", "fsdp", None)
    down_spec = P("ep", None, "fsdp")

    def per_device(layer_in, out_grad, expert_ids, gate_vals, w_one, w_two, w_three):
        tok, hidden = layer_in.shape
        top_k = expert_ids.shape[1]
        _, half, width = w_one.shape
        cap = capacity or capacity_of(tok, top_k, ep_size)
        chunks = cap // ROWS
        cube = (ring, ring, ring, ROWS, hidden)
        table = (ring, ring * ring, tok)
        small = (ring, ring, ring, 1, 128)
        vmem, dma = pltpu.VMEM, pltpu.SemaphoreType.DMA
        hbm = pl.BlockSpec(memory_space=pl.ANY)
        local = pl.BlockSpec(memory_space=pltpu.VMEM)
        sds = jax.ShapeDtypeStruct
        outs = pl.pallas_call(
            functools.partial(moe_kernel, ring, cap),
            out_shape=[
                sds((top_k, tok), F32), sds((tok, hidden), F32), sds(table, F32),
                *[sds((half, width), F32)] * 3,
                sds((2, chunks, *cube), BF16), sds((2, chunks, *cube), BF16),
                sds((chunks, *cube), BF16), sds((chunks, *cube), BF16), sds((chunks, *cube), BF16),
            ],
            in_specs=[hbm, hbm, local, local, hbm, hbm, hbm],
            out_specs=[local] + [hbm] * 10,
            scratch_shapes=[
                vmem((2, ring, tok, hidden), BF16), vmem((ring, tok, 128), BF16),
                *[vmem(table, F32)] * 6,
                *[vmem(small, F32)] * 8,
                vmem((2, 2, *cube), BF16), vmem((2, *cube), BF16), vmem((2, *cube), BF16), vmem(cube, BF16),
                vmem((tok, hidden), F32),
                vmem((2, half, 2 * width), BF16), vmem((2, half, width), BF16),
                vmem((2, half, 2 * width), F32), vmem((2, half, width), F32),
                *[vmem((half, width), F32)] * 3,
                dma((6,)), dma((7, 2)), dma((7, 2)), dma((7,)), dma((7,)), dma((3,)), dma((3,)), dma((3,)), dma((3,)),
                dma((3,)), dma((3,)), dma((3,)), dma((3,)),
                dma((2, 2, 3)), dma((2, chunks, 3)), dma((2, chunks, 3)),
                dma((2, chunks, 3)), dma((2, chunks, 3)),
                dma((2, 3)), dma((chunks, 3)), dma((chunks, 3)),
                dma((chunks, 3)), dma((chunks, 3)), dma((chunks, 3)), dma((chunks, 3)),
                dma((2,)), dma((3,)), dma((3,)), dma((3,)), dma((3,)), dma((2,)),
            ],
            compiler_params=pltpu.CompilerParams(
                collective_id=0, has_side_effects=True, vmem_limit_bytes=63 << 20
            ),
            name="moe_backward",
        )(layer_in, out_grad, expert_ids.T, gate_vals.T, w_one[0], w_three[0], w_two[0].T)
        dg, acc, places, g1, g3, g2 = outs[:6]
        dx, dg, g1, g3, g2 = pl.pallas_call(
            functools.partial(finish_kernel, ring, cap),
            out_shape=[sds((tok, hidden), BF16), sds((top_k, tok), F32), *[sds((half, width), F32)] * 3],
            in_specs=[hbm] * 9,
            out_specs=[hbm] * 5,
            scratch_shapes=[
                vmem((tok, hidden), F32), vmem(table, F32), vmem((3, half, width), F32), vmem(cube, BF16),
                vmem((tok, hidden), BF16), vmem((top_k, tok), F32), dma((7,)), dma((5,)),
            ],
            compiler_params=pltpu.CompilerParams(vmem_limit_bytes=63 << 20),
            name="moe_finish",
        )(dg, acc, places, g1, g3, g2, *outs[8:])
        return dx, dg.T, g1[None], g2.T[None], g3[None]

    return jax.shard_map(per_device, mesh=mesh,
                         in_specs=(tok_spec, tok_spec, tok_spec, tok_spec, up_spec, down_spec, up_spec),
                         out_specs=(tok_spec, tok_spec, up_spec, down_spec, up_spec), check_vma=False)


def solution(mesh):
    return build(mesh)
```

```python
import functools

import jax
import jax.numpy as jnp
from jax import lax
from jax.experimental import pallas as pl
from jax.experimental.pallas import tpu as pltpu
from jax.sharding import PartitionSpec as P

MESH = pl.DeviceIdType.MESH
ROWS = 16
BF16 = jnp.bfloat16
F32 = jnp.float32


def capacity_of(tok_dev, top_k, experts):
    return max(8, ((tok_dev * top_k * 5) // (4 * experts) + 7) // 8 * 8)


def column_groups(width, wide):
    tiles = width // 128
    base = tiles // 3
    sizes = [base + (tiles - 3 * base if p == wide else 0) for p in range(3)]
    starts = [sum(sizes[:p]) for p in range(3)]
    return [(128 * s, 128 * n) for s, n in zip(starts, sizes)]


def split_groups(width):
    base, spare = width // 384 * 128, width % 384
    even = [(0, base), (base, base), (2 * base, spare + base)]
    odd = [(0, base), (base, base + spare), (2 * base + spare, base)]
    return even, odd, (2 * base, spare)


def wait_bytes(ref, sem):
    pltpu.make_async_copy(ref, ref, sem).wait()


def dot(a, b, dims=((1,), (0,))):
    return lax.dot_general(a, b, (dims, ((), ())), preferred_element_type=F32)


def at(ref, lead, sel, col):
    return ref.at[(*lead, *(sel.get(a, slice(None)) for a in range(3)), slice(None), col)]


def one_hot(places, first):
    n, tok = places.shape
    row = lax.broadcasted_iota(jnp.int32, (n, ROWS, tok), 1) + first
    hit = places[:, None, :] == row.astype(F32)
    return jnp.where(hit, 1.0, 0.0).astype(BF16).reshape(n * ROWS, tok)


def returned_parts(ring, p):
    axis, rest = (p + 1) % 3, pl.ds(1, ring - 1)
    return ({p: 0, axis: 0}, {p: 0, axis: rest}, {p: rest})


def moe_kernel(ring, cap, x_hbm, u_hbm, ids_ref, gates_ref, w1_hbm, w3_hbm, w2_hbm,
               dg_out, acc_out, pos_out, g1_out, g3_out, g2_out, mid_hbm, fin_hbm, b1_hbm, b2_hbm, b3_hbm,
               xa, xe, pos0, pos1, pos2, sent0, sent1, sent2, line0, line1, line2, sg0, sg1, sg2, sg3, dg0, dg1, dg2, dg3,
               gbuf, xv, dxb, bv, acc, w13, w2, dw13, dw2, dw1r, dw3r, dw2r,
               ld_s, ag_s, ag_r, far_s, far_r, p_s, p_r, w_s, w_r, sg_s, sg_r, dg_s, dg_r,
               s2_s, s2_r, s2_l, s3_s, s3_r, r1_s, r1_r, r1_l, r2_s, r2_r, r3_s, r3_r,
               cl_s, bl_s, dw_s, dw_r, out_s, end_s):
    tok, hidden = x_hbm.shape
    top_k = ids_ref.shape[0]
    chunks = cap // ROWS
    plane = ring * ring
    block = plane * ROWS
    even, odd, spare = split_groups(hidden)
    spans = lambda groups: [pl.ds(s, n) for s, n in groups]
    even, odd, u_cols, cols = spans(even), spans(odd), spans(column_groups(hidden, 0)), spans(column_groups(hidden, 1))
    spare = pl.ds(*spare)
    pieces = [(0, 0, even[0]), (0, 1, even[1]), (0, 2, even[2])] + ([(0, 1, spare)] if spare.size else [])
    pieces += [(1, p, u_cols[p]) for p in range(3)]

    def held(i, d, part=slice(None), col=None):
        array, axis, whole = pieces[i]
        return xe.at[d, part] if i == 3 and spare.size else xa.at[array, d, part, col or whole]

    def by_chunk(array, c, body):
        if array == 1:
            body(u_cols)
        elif isinstance(c, int):
            body(odd if c % 2 else even)
        else:
            for parity, groups in enumerate((even, odd)):
                pl.when(lax.rem(c, 2) == parity)(functools.partial(body, groups))
    pos = (pos0, pos1, pos2)
    sent = (sent0, sent1, sent2)
    line = (line0, line1, line2)
    strides = (ring * ring, ring, 1)
    me = lax.axis_index("ep")
    core = lax.axis_index("fsdp")
    other = {"fsdp": 1 - core}
    coord = [lax.rem(me // s, ring) for s in strides]
    rest = pl.ds(1, ring - 1)
    width = w1_hbm.shape[1]
    one, three = pl.ds(0, width), pl.ds(width, width)
    weights = (lambda i: w13.at[i, :, one], lambda i: w13.at[i, :, three], lambda i: w2.at[i])

    def peer(axis, d):
        c = coord[axis]
        return {"ep": me + (lax.rem(c + d, ring) - c) * strides[axis]}

    def send(src, dst, s_sem, r_sem, device):
        pltpu.make_async_remote_copy(src_ref=src, dst_ref=dst, send_sem=s_sem, recv_sem=r_sem,
                                     device_id=device, device_id_type=MESH).start()

    def expert_column(order):
        row = lax.broadcasted_iota(jnp.int32, (ring ** 3, 1), 0)
        digits = (row // (ring * ring), lax.rem(row // ring, ring), lax.rem(row, ring))
        total = jnp.zeros_like(row)
        for digit, axis in zip(digits, order):
            total = total + lax.rem(digit + coord[axis], ring) * strides[axis]
        return total

    own = [
        pltpu.make_async_copy(x_hbm, xa.at[0, 0], ld_s.at[0]),
        pltpu.make_async_copy(u_hbm, xa.at[1, 0], ld_s.at[1]),
        *([pltpu.make_async_copy(x_hbm.at[:, spare], xe.at[0], ld_s.at[5])] if spare.size else []),
        pltpu.make_async_copy(w1_hbm, weights[0](core), ld_s.at[2]),
        pltpu.make_async_copy(w3_hbm, weights[1](core), ld_s.at[3]),
        pltpu.make_async_copy(w2_hbm, weights[2](core), ld_s.at[4]),
    ]
    for copy in own:
        copy.start()

    barrier = pltpu.get_barrier_semaphore()
    for axis in range(3):
        for d in range(1, ring):
            pl.semaphore_signal(barrier, inc=1, device_id=peer(axis, d), device_id_type=MESH)
    pl.semaphore_signal(barrier, inc=1, device_id=other, device_id_type=MESH)

    earlier = (lax.broadcasted_iota(jnp.int32, (tok, tok), 0) < lax.broadcasted_iota(jnp.int32, (tok, tok), 1))
    earlier = jnp.where(earlier, 1.0, 0.0).astype(BF16)
    for p, order in enumerate(((0, 1, 2), (1, 0, 2), (2, 0, 1))):
        expert = expert_column(order)
        chosen = jnp.zeros((ring ** 3, tok), F32)
        for j in range(top_k):
            chosen = chosen + jnp.where(ids_ref[j:j + 1, :] == expert, 1.0, 0.0)
        before = dot(chosen.astype(BF16), earlier)
        place = jnp.where((chosen > 0.5) & (before < cap), before, -1.0)
        pos[p][...] = place.reshape(ring, plane, tok)
        sent[p][...] = place.astype(BF16).reshape(ring, plane, tok)

    pltpu.make_async_copy(pos0, pos_out, end_s.at[0]).start()
    pl.semaphore_wait(barrier, 3 * (ring - 1) + 1)

    for p in range(3):
        for d in range(1, ring):
            send(sent[p].at[d], line[p].at[ring - d], p_s.at[p], p_r.at[p], peer(p, d))

    sides = sorted({1, ring - 1})

    for i, (array, axis, col) in enumerate(pieces):
        for d in sides:
            send((x_hbm, u_hbm)[array].at[:, col], held(i, ring - d), ag_s.at[i, d // 2], ag_r.at[i, (ring - d) // 2],
                 peer(axis, d))
    for i, src in enumerate((w1_hbm, w3_hbm, w2_hbm)):
        send(src, weights[i](core), w_s.at[i], w_r.at[i], other)

    expert = expert_column((0, 1, 2))
    place = pos0[...].reshape(ring ** 3, tok)
    gate = jnp.zeros((ring ** 3, tok), F32)
    for j in range(top_k):
        gate = gate + jnp.where(ids_ref[j:j + 1, :] == expert, gates_ref[j:j + 1, :], 0.0)
    lane = lax.broadcasted_iota(jnp.int32, (ring ** 3, 128), 1)

    def gate_place(i, table):
        for j in range(8):
            r = 8 * i + j
            picked = jnp.sum(jnp.where(place == r.astype(F32), gate, 0.0), axis=1, keepdims=True)
            table = jnp.where(lane == r, picked, table)
        return table

    table = lax.fori_loop(0, cap // 8, gate_place, jnp.zeros((ring ** 3, 128), F32))
    sg0[...] = table.reshape(ring, ring, ring, 1, 128)

    def small_start(axis, src, dst, s_sem, r_sem):
        sel = lambda i: tuple(i if a == axis else slice(None) for a in range(3))
        for d in range(1, ring):
            send(src.at[sel(d)], dst.at[sel(ring - d)], s_sem.at[axis], r_sem.at[axis], peer(axis, d))
        dst[sel(pl.ds(0, 1))] = src[sel(pl.ds(0, 1))]

    def small_wait(axis, dst, r_sem):
        wait_bytes(dst.at[tuple(rest if a == axis else slice(None) for a in range(3))], r_sem.at[axis])

    small_start(0, sg0, sg1, sg_s, sg_r)
    for ref in (dw13, dw2, acc, dg0):
        ref[...] = jnp.zeros_like(ref)
    for i, (array, axis, col) in enumerate(pieces):
        for d in sides:
            wait_bytes(held(i, d), ag_r.at[i, d // 2])
            if ring == 4:
                part = pl.ds((d // 2) * (tok // 2), tok // 2)
                send(held(i, d, part), held(i, 2, part), far_s.at[i], far_r.at[i], peer(axis, ring - d))
    for copy in own:
        copy.wait()
    for p in range(3):
        wait_bytes(line[p].at[rest], p_r.at[p])

    def dispatch(c):
        for array in range(2):
            by_chunk(array, c, functools.partial(dispatch_stream, c, array))

    def dispatch_stream(c, array, groups):
        slot = lax.rem(c, 2)
        for p in range(3):
            axis, col = (p + 1) % 3, groups[p]
            mine = [i for i, piece in enumerate(pieces) if piece[:2] == (array, p)]
            for i in mine:
                if ring == 4:
                    @pl.when(c == 0)
                    def _():
                        wait_bytes(held(i, 2), far_r.at[i])

            @pl.when(c >= 2)
            def _():
                wait_bytes(at(gbuf, (array, slot), {axis: rest}, col), s2_s.at[array, slot, p])

            for d in range(ring):
                hot = one_hot(pos[p][0] if d == 0 else line[p][d].astype(F32), c * ROWS)
                for i in mine:
                    first = max(pieces[i][2].start, col.start)
                    end = min(pieces[i][2].start + pieces[i][2].size, col.start + col.size)
                    if first >= end:
                        continue
                    own_col = pl.ds(first, end - first)
                    rows = dot(hot, held(i, d, col=own_col)[...]).astype(BF16)
                    idx = tuple(d if a == p else slice(None) for a in range(3))
                    gbuf[(array, slot, *idx, slice(None), own_col)] = rows.reshape(ring, ring, ROWS, own_col.size)
            for d in range(1, ring):
                send(at(gbuf, (array, slot), {axis: d}, col), at(mid_hbm, (array, c), {axis: ring - d}, col),
                     s2_s.at[array, slot, p], s2_r.at[array, c, p], peer(axis, d))
            pltpu.make_async_copy(at(gbuf, (array, slot), {axis: 0}, col),
                                  at(mid_hbm, (array, c), {axis: 0}, col), s2_l.at[array, c, p]).start()

    def forward(c):
        for array in range(2):
            by_chunk(array, c, functools.partial(forward_stream, c, array))

    def forward_stream(c, array, groups):
        for p, col in enumerate(groups):
            axis, last = (p + 1) % 3, (p + 2) % 3
            wait_bytes(at(mid_hbm, (array, c), {axis: rest}, col), s2_r.at[array, c, p])
            wait_bytes(at(mid_hbm, (array, c), {axis: 0}, col), s2_l.at[array, c, p])
            for d in range(1, ring):
                send(at(mid_hbm, (array, c), {last: d}, col), at(fin_hbm, (array, c), {last: ring - d}, col),
                     s3_s.at[array, c, p], s3_r.at[array, c, p], peer(last, d))

    def load_stream(c, array, groups):
        for p, col in enumerate(groups):
            last = (p + 2) % 3
            wait_bytes(at(fin_hbm, (array, c), {last: rest}, col), s3_r.at[array, c, p])
            for src, part in ((fin_hbm, rest), (mid_hbm, 0)):
                pltpu.make_async_copy(at(src, (array, c), {last: part}, col),
                                      at(xv, (array,), {last: part}, col), cl_s.at[array]).start()

    def compute(c):
        slot = lax.rem(c, 2)
        for array in range(2):
            by_chunk(array, c, functools.partial(load_stream, c, array))

        @pl.when(c >= 2)
        def _():
            for p in range(3):
                wait_bytes(at(dxb, (slot,), {(p + 2) % 3: rest}, cols[p]), r1_s.at[slot, p])

        for array in range(2):
            wait_bytes(xv.at[array], cl_s.at[array])

        def step(i, carry):
            slabs = pl.ds(2 * i, 2)
            x = xv[0, slabs].reshape(2 * block, hidden)
            u = xv[1, slabs].reshape(2 * block, hidden)
            w13_full = w13[...].reshape(hidden, 2 * width)
            hit = (lax.broadcasted_iota(jnp.int32, (2 * plane, ROWS, 128), 2)
                   == lax.broadcasted_iota(jnp.int32, (2 * plane, ROWS, 128), 1) + c * ROWS)
            s = sg3[slabs].reshape(2 * plane, 1, 128)
            s = jnp.sum(jnp.where(hit, s, 0.0), axis=2, keepdims=True).reshape(2 * block, 1)
            h13 = dot(x, w13_full)
            h1, h3 = h13[:, :width], h13[:, width:]
            sig = jax.nn.sigmoid(h1)
            silu = h1 * sig
            act = (silu * h3).astype(BF16)
            u32 = u.astype(F32)
            g = (s * u32).astype(BF16)
            w2_full = w2[...].reshape(hidden, width)
            y = dot(act, w2_full, ((1,), (1,)))
            dg = jnp.sum(u32 * y, axis=1, keepdims=True)
            da = dot(g, w2_full)
            dw2[...] += dot(g, act, ((0,), (0,))).reshape(dw2.shape)
            dh1 = (da * h3 * sig * (1.0 + h1 * (1.0 - sig))).astype(BF16)
            dh3 = (da * silu).astype(BF16)
            dh13 = jnp.concatenate([dh1, dh3], axis=1)
            dx = dot(dh13, w13_full, ((1,), (1,)))
            dxb[slot, slabs] = dx.astype(BF16).reshape(2, ring, ring, ROWS, hidden)
            dw13[...] += dot(x, dh13, ((0,), (0,))).reshape(dw13.shape)
            spread = jnp.sum(jnp.where(hit, dg.reshape(2 * plane, ROWS, 1), 0.0), axis=1, keepdims=True)
            dg0[slabs] += spread.reshape(2, ring, ring, 1, 128)
            for j in range(2):
                return_slab(2 * i + j)
            return carry

        def return_slab(m):
            for p in range(3):
                last = (p + 2) % 3

                def start(here, there, device):
                    src, dst = at(dxb, (slot,), here, cols[p]), at(b1_hbm, (c,), there, cols[p])
                    if device is None:
                        pltpu.make_async_copy(src, dst, r1_l.at[c, p]).start()
                    else:
                        send(src, dst, r1_s.at[slot, p], r1_r.at[c, p], device)

                if last == 0:
                    @pl.when(m > 0)
                    def _():
                        start({0: m}, {0: ring - m}, peer(0, m))

                    @pl.when(m == 0)
                    def _():
                        start({0: 0}, {0: 0}, None)
                else:
                    for d in range(1, ring):
                        start({0: m, last: d}, {0: m, last: ring - d}, peer(last, d))
                    start({0: m, last: 0}, {0: m, last: 0}, None)

        lax.fori_loop(0, ring // 2, step, 0)

    def back_two(c):
        for p in range(3):
            axis, last = (p + 1) % 3, (p + 2) % 3
            wait_bytes(at(b1_hbm, (c,), {last: rest}, cols[p]), r1_r.at[c, p])
            wait_bytes(at(b1_hbm, (c,), {last: 0}, cols[p]), r1_l.at[c, p])
            for d in range(1, ring):
                send(at(b1_hbm, (c,), {axis: d}, cols[p]), at(b2_hbm, (c,), {axis: ring - d}, cols[p]),
                     r2_s.at[c, p], r2_r.at[c, p], peer(axis, d))

    def back_three(c):
        for p in range(3):
            axis = (p + 1) % 3
            wait_bytes(at(b2_hbm, (c,), {axis: rest}, cols[p]), r2_r.at[c, p])
            for d in range(1, ring):
                for src, part in ((b2_hbm, rest), (b1_hbm, 0)):
                    send(at(src, (c,), {p: d, axis: part}, cols[p]),
                         at(b3_hbm, (c,), {p: ring - d, axis: part}, cols[p]),
                         r3_s.at[c, p], r3_r.at[c, p], peer(p, d))

    def combine(c):
        for p in range(3):
            wait_bytes(at(b3_hbm, (c,), {p: rest}, cols[p]), r3_r.at[c, p])
            for src, sel in zip((b1_hbm, b2_hbm, b3_hbm), returned_parts(ring, p)):
                pltpu.make_async_copy(at(src, (c,), sel, cols[p]), at(bv, (), sel, cols[p]), bl_s.at[p]).start()
        for p in range(3):
            wait_bytes(at(bv, (), {}, cols[p]), bl_s.at[p])

        def step(m, carry):
            acc[...] += dot(one_hot(pos0[m], c * ROWS), bv[m].reshape(block, hidden), ((0,), (0,)))
            return carry

        lax.fori_loop(0, ring, step, 0)

    grads = (
        (lambda i: dw13.at[i, :, one], dw1r, g1_out),
        (lambda i: dw13.at[i, :, three], dw3r, g3_out),
        (lambda i: dw2.at[i], dw2r, g2_out),
    )

    def gate_grads():
        small_wait(0, dg3, dg_r)
        expert = expert_column((0, 1, 2))
        place = pos0[...].reshape(ring ** 3, tok)
        values = dg3[...].reshape(ring ** 3, 128)

        def pick(i, total):
            for j in range(8):
                r = 8 * i + j
                value = jnp.sum(jnp.where(lane == r, values, 0.0), axis=1, keepdims=True)
                total = total + jnp.where(place == r.astype(F32), value, 0.0)
            return total

        dense = lax.fori_loop(0, cap // 8, pick, jnp.zeros((ring ** 3, tok), F32))
        for j in range(top_k):
            dg_out[j:j + 1, :] = jnp.sum(jnp.where(ids_ref[j:j + 1, :] == expert, dense, 0.0), axis=0, keepdims=True)

    def tick(k, carry):
        @pl.when(k < chunks)
        def _():
            dispatch(k)

        @pl.when(k == 0)
        def _():
            small_wait(0, sg1, sg_r)
            small_start(1, sg1, sg2, sg_s, sg_r)

        @pl.when(k == 1)
        def _():
            small_wait(1, sg2, sg_r)
            small_start(2, sg2, sg3, sg_s, sg_r)

        @pl.when((k >= 1) & (k <= chunks))
        def _():
            forward(k - 1)

        @pl.when(k == 2)
        def _():
            small_wait(2, sg3, sg_r)
            for i in range(3):
                wait_bytes(weights[i](1 - core), w_r.at[i])

        @pl.when(k >= 2)
        def _():
            compute(k - 2)

        @pl.when(k == chunks + 1)
        def _():
            small_start(2, dg0, dg1, dg_s, dg_r)
            for i, (mine, theirs, _) in enumerate(grads):
                send(mine(1 - core), theirs, dw_s.at[i], dw_r.at[i], other)

        @pl.when(k >= 3)
        def _():
            back_two(k - 3)

        @pl.when((k >= 4) & (k <= chunks))
        def _():
            back_three(k - 4)

        @pl.when((k >= 5) & (k <= chunks))
        def _():
            combine(k - 5)

        return carry

    lax.fori_loop(0, chunks + 2, tick, 0)
    last_one = chunks - 1
    small_wait(2, dg1, dg_r)
    small_start(1, dg1, dg2, dg_s, dg_r)
    back_two(last_one)
    back_three(last_one - 2)
    combine(last_one - 3)
    back_three(last_one - 1)
    small_wait(1, dg2, dg_r)
    small_start(0, dg2, dg3, dg_s, dg_r)
    back_three(last_one)
    for i, (mine, theirs, out) in enumerate(grads):
        wait_bytes(theirs, dw_r.at[i])
        theirs[...] += mine(core)[...]
        pltpu.make_async_copy(theirs, out, out_s.at[i]).start()
    combine(last_one - 2)
    gate_grads()
    combine(last_one - 1)
    pltpu.make_async_copy(acc, acc_out, end_s.at[1]).start()

    for i in range(len(pieces)):
        for d in sides:
            wait_bytes(held(i, d), ag_s.at[i, d // 2])
        if ring == 4:
            wait_bytes(held(i, 2), far_s.at[i])
    for p in range(3):
        wait_bytes(line[p].at[rest], p_s.at[p])
        wait_bytes(sg1.at[rest], sg_s.at[p])
        wait_bytes(dg1.at[rest], dg_s.at[p])
    for i in range(3):
        wait_bytes(weights[i](1 - core), w_s.at[i])
    for i, (mine, theirs, out) in enumerate(grads):
        wait_bytes(theirs, dw_s.at[i])
        wait_bytes(out, out_s.at[i])
    for slot in range(2):
        for p in range(3):
            axis, last = (p + 1) % 3, (p + 2) % 3
            for array in range(2):
                by_chunk(array, slot, lambda groups: wait_bytes(
                    at(gbuf, (array, slot), {axis: rest}, groups[p]), s2_s.at[array, slot, p]))
            wait_bytes(at(dxb, (slot,), {last: rest}, cols[p]), r1_s.at[slot, p])

    def drain(c, carry):
        for p in range(3):
            axis, last = (p + 1) % 3, (p + 2) % 3
            for array in range(2):
                by_chunk(array, c, lambda groups: wait_bytes(
                    at(fin_hbm, (array, c), {last: rest}, groups[p]), s3_s.at[array, c, p]))
            wait_bytes(at(b2_hbm, (c,), {axis: rest}, cols[p]), r2_s.at[c, p])
            wait_bytes(at(b3_hbm, (c,), {p: rest}, cols[p]), r3_s.at[c, p])
        return carry

    lax.fori_loop(0, chunks, drain, 0)
    wait_bytes(pos_out, end_s.at[0])
    wait_bytes(acc_out, end_s.at[1])
    for p in range(3):
        wait_bytes(at(b3_hbm, (last_one,), {p: rest}, cols[p]), r3_r.at[last_one, p])


def finish_kernel(ring, cap, dg_hbm, acc_hbm, pos_hbm, g1_hbm, g3_hbm, g2_hbm, b1_hbm, b2_hbm, b3_hbm,
                  dx_hbm, dg_out, g1_out, g3_out, g2_out, acc, pos, grad, bv, dx, dg, in_s, out_s):
    hidden = acc.shape[1]
    chunk = cap // ROWS - 1
    cols = [pl.ds(s, n) for s, n in column_groups(hidden, 1)]
    pltpu.make_async_copy(pos_hbm, pos, in_s.at[0]).start()
    for p in range(3):
        for src, sel in zip((b1_hbm, b2_hbm, b3_hbm), returned_parts(ring, p)):
            pltpu.make_async_copy(at(src, (chunk,), sel, cols[p]), at(bv, (), sel, cols[p]), in_s.at[1]).start()
    pltpu.make_async_copy(acc_hbm, acc, in_s.at[2]).start()
    for i, src in enumerate((g1_hbm, g3_hbm, g2_hbm)):
        pltpu.make_async_copy(src, grad.at[i], in_s.at[3 + i]).start()
    pltpu.make_async_copy(dg_hbm, dg, in_s.at[6]).start()
    wait_bytes(pos, in_s.at[0])
    wait_bytes(bv, in_s.at[1])
    wait_bytes(acc, in_s.at[2])
    for m in range(ring):
        block = ring * ring * ROWS
        acc[...] += dot(one_hot(pos[m], chunk * ROWS), bv[m].reshape(block, hidden), ((0,), (0,)))
        if m < 3:
            wait_bytes(grad.at[m], in_s.at[3 + m])
            pltpu.make_async_copy(grad.at[m], (g1_out, g3_out, g2_out)[m], out_s.at[m]).start()
    for m in range(ring, 3):
        wait_bytes(grad.at[m], in_s.at[3 + m])
        pltpu.make_async_copy(grad.at[m], (g1_out, g3_out, g2_out)[m], out_s.at[m]).start()
    wait_bytes(dg, in_s.at[6])
    pltpu.make_async_copy(dg, dg_out, out_s.at[4]).start()
    dx[...] = acc[...].astype(BF16)
    copy = pltpu.make_async_copy(dx, dx_hbm, out_s.at[3])
    copy.start()
    for m, out in enumerate((g1_out, g3_out, g2_out)):
        wait_bytes(out, out_s.at[m])
    wait_bytes(dg_out, out_s.at[4])
    copy.wait()


def build(mesh, capacity=None):
    ep_size = mesh.shape["ep"]
    ring = round(ep_size ** (1 / 3))
    tok_spec = P(("fsdp", "ep"), None)
    up_spec = P("ep", "fsdp", None)
    down_spec = P("ep", None, "fsdp")

    def per_device(layer_in, out_grad, expert_ids, gate_vals, w_one, w_two, w_three):
        tok, hidden = layer_in.shape
        top_k = expert_ids.shape[1]
        _, half, width = w_one.shape
        cap = capacity or capacity_of(tok, top_k, ep_size)
        chunks = cap // ROWS
        cube = (ring, ring, ring, ROWS, hidden)
        table = (ring, ring * ring, tok)
        small = (ring, ring, ring, 1, 128)
        vmem, dma = pltpu.VMEM, pltpu.SemaphoreType.DMA
        hbm = pl.BlockSpec(memory_space=pl.ANY)
        local = pl.BlockSpec(memory_space=pltpu.VMEM)
        sds = jax.ShapeDtypeStruct
        outs = pl.pallas_call(
            functools.partial(moe_kernel, ring, cap),
            out_shape=[
                sds((top_k, tok), F32), sds((tok, hidden), F32), sds(table, F32),
                *[sds((half, width), F32)] * 3,
                sds((2, chunks, *cube), BF16), sds((2, chunks, *cube), BF16),
                sds((chunks, *cube), BF16), sds((chunks, *cube), BF16), sds((chunks, *cube), BF16),
            ],
            in_specs=[hbm, hbm, local, local, hbm, hbm, hbm],
            out_specs=[local] + [hbm] * 10,
            scratch_shapes=[
                vmem((2, ring, tok, hidden), BF16), vmem((ring, tok, 128), BF16),
                *[vmem(table, F32)] * 3, *[vmem(table, BF16)] * 6,
                *[vmem(small, F32)] * 8,
                vmem((2, 2, *cube), BF16), vmem((2, *cube), BF16), vmem((2, *cube), BF16), vmem(cube, BF16),
                vmem((tok, hidden), F32),
                vmem((2, half, 2 * width), BF16), vmem((2, half, width), BF16),
                vmem((2, half, 2 * width), F32), vmem((2, half, width), F32),
                *[vmem((half, width), F32)] * 3,
                dma((6,)), dma((7, 2)), dma((7, 2)), dma((7,)), dma((7,)), dma((3,)), dma((3,)), dma((3,)), dma((3,)),
                dma((3,)), dma((3,)), dma((3,)), dma((3,)),
                dma((2, 2, 3)), dma((2, chunks, 3)), dma((2, chunks, 3)),
                dma((2, chunks, 3)), dma((2, chunks, 3)),
                dma((2, 3)), dma((chunks, 3)), dma((chunks, 3)),
                dma((chunks, 3)), dma((chunks, 3)), dma((chunks, 3)), dma((chunks, 3)),
                dma((2,)), dma((3,)), dma((3,)), dma((3,)), dma((3,)), dma((2,)),
            ],
            compiler_params=pltpu.CompilerParams(
                collective_id=0, has_side_effects=True, vmem_limit_bytes=63 << 20
            ),
            name="moe_backward",
        )(layer_in, out_grad, expert_ids.T, gate_vals.T, w_one[0], w_three[0], w_two[0].T)
        dg, acc, places, g1, g3, g2 = outs[:6]
        dx, dg, g1, g3, g2 = pl.pallas_call(
            functools.partial(finish_kernel, ring, cap),
            out_shape=[sds((tok, hidden), BF16), sds((top_k, tok), F32), *[sds((half, width), F32)] * 3],
            in_specs=[hbm] * 9,
            out_specs=[hbm] * 5,
            scratch_shapes=[
                vmem((tok, hidden), F32), vmem(table, F32), vmem((3, half, width), F32), vmem(cube, BF16),
                vmem((tok, hidden), BF16), vmem((top_k, tok), F32), dma((7,)), dma((5,)),
            ],
            compiler_params=pltpu.CompilerParams(vmem_limit_bytes=63 << 20),
            name="moe_finish",
        )(dg, acc, places, g1, g3, g2, *outs[8:])
        return dx, dg.T, g1[None], g2.T[None], g3[None]

    return jax.shard_map(per_device, mesh=mesh,
                         in_specs=(tok_spec, tok_spec, tok_spec, tok_spec, up_spec, down_spec, up_spec),
                         out_specs=(tok_spec, tok_spec, up_spec, down_spec, up_spec), check_vma=False)


def solution(mesh):
    return build(mesh)
```
